32 devices in a mesh: seq: 8 (over z, y), tp: 4 (over x, core).
Axes of the slice: x: 2, y: 2, z: 4, core: 2. Of those that a mesh axis runs over, the one named last changes fastest.
Arguments:
- queries: bfloat16 [1, 2048, 4096], P(None, 'seq', 'tp'), may hold values from -13 to 13
- key_rows: bfloat16 [1, 2048, 2048], P(None, 'seq', 'tp'), may hold values from -13 to 13
- value_rows: bfloat16 [1, 2048, 2048], P(None, 'seq', 'tp'), may hold values from -6 to 6
- residual: bfloat16 [1, 2048, 3584], P(None, 'seq', 'tp'), may hold values from -6 to 6
- out_weight: bfloat16 [4096, 3584], P('tp')
- post_scale: float32 [3584], P('tp'), may hold values from 0.1 to 1.9
- lengths: int32 [1], replicated, may hold values from 512 to 2047
- owners: int32 [1, 8], replicated, may hold values from 0 to 7, each once within a row
Outputs:
- hidden_out: bfloat16 [1, 2048, 3584], P(None, 'seq', 'tp')
- cache_keys: bfloat16 [1, 4096, 2048], P(None, 'seq', 'tp')
- cache_values: bfloat16 [1, 4096, 2048], P(None, 'seq', 'tp')
The draws below stay inside these ranges and needn't reach their ends.
Inputs may be any that keep to these rules, and one draw needn't show every extreme that they name: Each row of owners names every number from 0 to 7 once.
All inputs are finite; a program needn't handle non-finite values.
Results may differ from the reference program's by a relative error of at most 0.0083.
Values may be sent and summed in bfloat16 or wider, within the bound.
A program may use at most 64 MiB of HBM per device.

```python
import jax
import jax.numpy as jnp
from jax import lax

D = 3584
QH = 16
KVH = 8
HD = 256
WINDOW = 4096
SEQS = 1
SHARD = 256
LENGTH = 2048
N_SEQ = 8


def draw_out_weight(key, part):
    entry_key, jitter_key = jax.random.split(jax.random.fold_in(key, 17))
    fan_in = QH * HD
    entries = jax.random.normal(entry_key, (fan_in, D), jnp.float32)
    rising = jnp.exp(jnp.linspace(jnp.log(0.5), jnp.log(5.0), D)).astype(jnp.float32)
    jitter = jnp.exp(jax.random.uniform(jitter_key, (D,), jnp.float32, -0.35, 0.35))
    return (entries * (rising * jitter)[None, :] * fan_in ** (-0.5)).astype(jnp.bfloat16)


def planted_lift(key):
    mask_key, scale_key, sign_key = jax.random.split(jax.random.fold_in(key, 29), 3)
    fraction = 0.03
    chosen = jax.random.bernoulli(mask_key, fraction, (SEQS, LENGTH))
    amplitude = jax.random.uniform(scale_key, (SEQS, LENGTH), jnp.float32, 8.0, 13.5) * HD ** 0.25
    raised = jnp.where(chosen, amplitude, jnp.zeros_like(amplitude))
    directions = jax.random.rademacher(sign_key, (KVH, HD), jnp.float32) * HD ** (-0.5)
    return (raised, directions)


def background_rows(noise_key, width):
    background = jnp.clip(jax.random.normal(noise_key, (SEQS, LENGTH, width), jnp.float32), -6.0, 6.0)
    return background


def draw_queries(key, part):
    raised, directions = planted_lift(key)
    background = background_rows(jax.random.fold_in(key, 31), QH * HD)
    repeated = jnp.repeat(directions, QH // KVH, axis=0).reshape(QH * HD)
    return (background + raised[:, :, None] * repeated[None, None, :]).astype(jnp.bfloat16)


def draw_key_rows(key, part):
    raised, directions = planted_lift(key)
    background = background_rows(jax.random.fold_in(key, 37), KVH * HD)
    flattened = directions.reshape(KVH * HD)
    return (background + raised[:, :, None] * flattened[None, None, :]).astype(jnp.bfloat16)


def shard_levels(stream_key, dims, shards, smallest, high):
    def one(dim, parts):
        heights = jax.random.uniform(jax.random.fold_in(jax.random.fold_in(stream_key, 6), dim), (parts,), jnp.float32, smallest / len(shards), high / len(shards))
        return jnp.repeat(jnp.exp(heights), dims[dim] // parts).reshape((-1,) + (1,) * (len(dims) - dim - 1))

    loudness = one(*shards[0])
    for cut in shards[1:]:
        loudness = loudness * one(*cut)
    return loudness


def scatter_about(own_key, extent, scale, most, pieces=(), kind=jnp.bfloat16):
    loudness = shard_levels(own_key, extent, pieces, -0.22, 0.18) if pieces else 1.0
    values = jax.random.normal(own_key, extent, jnp.float32) * scale * loudness
    return jnp.minimum(jnp.maximum(values, -most), most).astype(kind)


def setup_inputs(seed: int = 0) -> dict:
    keys = jax.random.split(jax.random.key(seed), 9)
    queries = draw_queries(jax.random.fold_in(keys[8], 71), 0)
    key_rows = draw_key_rows(jax.random.fold_in(keys[8], 71), 0)
    value_rows = scatter_about(keys[2], (SEQS, LENGTH, KVH * HD), 1.0, 6.0, ((1, 8), (2, 4)))
    residual = scatter_about(keys[3], (SEQS, LENGTH, D), 1.0, 6.0, ((1, 8), (2, 4)))
    out_weight = draw_out_weight(jax.random.fold_in(keys[8], 71), 0)
    post_scale = jnp.clip(1.0 + 0.18 * jax.random.normal(keys[5], (D,), jnp.float32), 0.1, 1.9)
    lengths = jax.random.randint(keys[6], (SEQS,), min(WINDOW, LENGTH) // 4, min(WINDOW, LENGTH)).astype(jnp.int32)
    owners = jax.vmap(lambda own: jax.random.permutation(own, N_SEQ))(jax.random.split(keys[7], SEQS)).reshape((SEQS, N_SEQ)).astype(jnp.int32)
    return {"queries": queries, "key_rows": key_rows, "value_rows": value_rows, "residual": residual, "out_weight": out_weight, "post_scale": post_scale, "lengths": lengths, "owners": owners}


soft_cap = 50.0
norm_eps = 1e-06

def attend_rows(queries, padded_keys, padded_values, row_start):
    group_size = QH // KVH
    query_block = lax.dynamic_slice_in_dim(queries, row_start, SHARD, 1).astype(jnp.float32).reshape(SEQS, SHARD, KVH, group_size, HD)
    key_block = lax.dynamic_slice_in_dim(padded_keys, row_start, WINDOW + SHARD, 1).astype(jnp.float32).reshape(SEQS, WINDOW + SHARD, KVH, HD)
    value_block = lax.dynamic_slice_in_dim(padded_values, row_start, WINDOW + SHARD, 1).astype(jnp.float32).reshape(SEQS, WINDOW + SHARD, KVH, HD)
    scores = jnp.einsum('sqhgd,skhd->shgqk', query_block, key_block) * HD ** (-0.5)
    capped = soft_cap * jnp.tanh(scores / soft_cap)
    query_pos = row_start + jnp.arange(SHARD, dtype=jnp.int32)
    key_pos = row_start - WINDOW + jnp.arange(WINDOW + SHARD, dtype=jnp.int32)
    spread = query_pos[:, None] - key_pos[None, :]
    live_mask = (spread >= 0) & (spread < WINDOW) & (key_pos[None, :] >= 0)
    weights = jnp.where(live_mask, jnp.exp(capped), jnp.zeros_like(capped))
    totals = lax.optimization_barrier(jnp.sum(weights, axis=-1))
    rounded = lax.optimization_barrier(weights.astype(jnp.bfloat16)).astype(jnp.float32)
    mixture = jnp.einsum('shgqk,skhd->sqhgd', rounded, value_block)
    attended = mixture / jnp.transpose(totals, (0, 3, 1, 2))[..., None]
    return attended.astype(jnp.bfloat16).reshape(SEQS, SHARD, QH * HD)

def window_rows(rows_in, length):
    slots = jnp.arange(WINDOW, dtype=jnp.int32)
    anchor = length - WINDOW + jnp.mod(slots - length + WINDOW, WINDOW)
    taken = jnp.take(rows_in, jnp.clip(anchor, 0, LENGTH - 1), axis=0)
    return jnp.where((anchor >= 0)[:, None], taken, jnp.zeros_like(taken))

def owner_layout(slotted, owner_row):
    devices = jnp.arange(N_SEQ, dtype=jnp.int32)
    matches = owner_row[:, None] == devices[None, :]
    inverse = lax.optimization_barrier(jnp.sum(jnp.where(matches, devices[:, None], jnp.zeros_like(devices)[:, None]), axis=0))
    local = jnp.arange(WINDOW // N_SEQ, dtype=jnp.int32)
    block_rows = SHARD // N_SEQ
    chosen = local[None, :] // block_rows * SHARD + inverse[:, None] * block_rows + local[None, :] % block_rows
    return jnp.take(slotted, chosen.reshape(-1), axis=0)

def reference(queries, key_rows, value_rows, residual, out_weight, post_scale, lengths, owners):
    front = jnp.zeros((SEQS, WINDOW, KVH * HD), key_rows.dtype)
    padded_keys = jnp.concatenate([front, key_rows], axis=1)
    padded_values = jnp.concatenate([front, value_rows], axis=1)
    starts = jnp.arange(LENGTH // SHARD, dtype=jnp.int32) * SHARD
    blocks = lax.map(lambda row_start: attend_rows(queries, padded_keys, padded_values, row_start), starts)
    attended = jnp.transpose(blocks, (1, 0, 2, 3)).reshape(SEQS * LENGTH, QH * HD)
    branch = jnp.dot(attended, out_weight, preferred_element_type=jnp.float32)
    mean_square = lax.optimization_barrier(jnp.mean(branch * branch, axis=-1, keepdims=True))
    normed = branch * lax.rsqrt(mean_square + norm_eps) * post_scale
    hidden_out = (residual.reshape(SEQS * LENGTH, D).astype(jnp.float32) + normed).astype(jnp.bfloat16).reshape(SEQS, LENGTH, D)
    cache_keys = jnp.stack([owner_layout(window_rows(key_rows[seq_index], lengths[seq_index]), owners[seq_index]) for seq_index in range(SEQS)])
    cache_values = jnp.stack([owner_layout(window_rows(value_rows[seq_index], lengths[seq_index]), owners[seq_index]) for seq_index in range(SEQS)])
    return (hidden_out, cache_keys, cache_values)
```

```python
import functools

import jax
import jax.numpy as jnp
from jax import lax
from jax.experimental import pallas as pl
from jax.experimental.pallas import tpu as pltpu
from jax.sharding import PartitionSpec as P

D = 3584
HD = 256
WINDOW = 4096
MESH = pl.DeviceIdType.MESH
LOG2E = 1.4426950408889634
ROWS = 128


soft_cap = 50.0
norm_eps = 1e-06


def shifted(x, axis, by):
    peers = lax.axis_size(axis)
    pairs = [(i, i + by) for i in range(peers) if 0 <= i + by < peers]
    return lax.ppermute(x, axis, pairs)


def attend_block(grouped, block_keys, block_values, query_pos, key_pos, state_pair):
    numerator, denominator = state_pair
    seq_count, query_count, kv_local, group_size, head_size = grouped.shape
    keyed_rows = block_keys.reshape(seq_count, block_keys.shape[1], kv_local, head_size)
    valued_rows = block_values.reshape(seq_count, block_values.shape[1], kv_local, head_size)
    scores = jnp.einsum(
        "sqhgd,skhd->shgqk", grouped, keyed_rows, preferred_element_type=jnp.float32
    ) * head_size ** (-0.5)
    capped = soft_cap * jnp.tanh(scores / soft_cap)
    spread = query_pos[:, None] - key_pos[None, :]
    live_mask = (spread >= 0) & (spread < WINDOW) & (key_pos[None, :] >= 0)
    weights = jnp.where(live_mask, jnp.exp(capped), jnp.zeros_like(capped))
    denominator = denominator + jnp.sum(weights, axis=-1)
    numerator = numerator + jnp.einsum(
        "shgqk,skhd->sqhgd",
        weights.astype(jnp.bfloat16),
        valued_rows,
        preferred_element_type=jnp.float32,
    )
    return (numerator, denominator)


def reorder_blocks(blocked, ordering):
    return blocked[ordering]


def local(queries, key_rows, value_rows, residual, out_weight, post_scale, lengths, owners):
    seq_count, shard_len, query_width = queries.shape
    seq_size = lax.axis_size("seq")
    if (
        seq_count == 1 and lax.axis_size("tp") == 4 and seq_size % 2 == 0 and seq_size >= 4
        and seq_size * shard_len <= WINDOW and key_rows.shape[2] == 2 * HD
    ):
        return fused(
            seq_size, queries, key_rows, value_rows, residual, out_weight, post_scale, lengths,
            owners,
        )
    kv_width = key_rows.shape[2]
    kv_local = kv_width // HD
    group_size = query_width // kv_width
    grouped = queries.reshape(seq_count, shard_len, kv_local, group_size, HD)
    position = lax.axis_index("seq")
    seq_devices = lax.axis_size("seq")
    offsets = jnp.arange(shard_len, dtype=jnp.int32)
    query_pos = position * shard_len + offsets
    numerator = jnp.zeros((seq_count, shard_len, kv_local, group_size, HD), jnp.float32)
    denominator = jnp.zeros((seq_count, kv_local, group_size, shard_len), jnp.float32)
    state_pair = attend_block(
        grouped, key_rows, value_rows, query_pos, query_pos, (numerator, denominator)
    )
    hop_count = min(WINDOW // shard_len, seq_devices - 1)
    arrived = []
    current = (key_rows, value_rows)
    for hop_index in range(1, hop_count + 1):
        current = shifted((current[0], current[1]), "seq", 1)
        arrived.append((hop_index, current))
        if len(arrived) == 2 or hop_index == hop_count:
            ordered = arrived[::-1]
            block_keys = jnp.concatenate([member[1][0] for member in ordered], axis=1)
            block_values = jnp.concatenate([member[1][1] for member in ordered], axis=1)
            block_pos = jnp.concatenate(
                [(position - member[0]) * shard_len + offsets for member in ordered]
            )
            state_pair = attend_block(
                grouped, block_keys, block_values, query_pos, block_pos, state_pair
            )
            arrived = []
    numerator, denominator = state_pair
    attended = (numerator / jnp.transpose(denominator, (0, 3, 1, 2))[..., None]).astype(
        jnp.bfloat16
    )
    partial_value = jnp.dot(
        attended.reshape(seq_count * shard_len, query_width),
        out_weight,
        preferred_element_type=jnp.float32,
    )
    partial_value = partial_value.reshape(seq_count, shard_len, out_weight.shape[1])
    branch = lax.psum_scatter(partial_value, "tp", scatter_dimension=2, tiled=True)
    squares = lax.psum(jnp.sum(branch * branch, axis=-1), "tp")
    normed = branch * lax.rsqrt(squares / D + norm_eps)[..., None] * post_scale
    hidden_out = (residual.astype(jnp.float32) + normed).astype(jnp.bfloat16)
    block_rows = shard_len // seq_devices
    slot_span = WINDOW // shard_len
    live_rows = (query_pos[None, :] >= lengths[:, None] - WINDOW) & (
        query_pos[None, :] < lengths[:, None]
    )
    kept_keys = jnp.where(live_rows[..., None], key_rows, jnp.zeros_like(key_rows))
    kept_values = jnp.where(live_rows[..., None], value_rows, jnp.zeros_like(value_rows))
    devices = jnp.arange(seq_devices, dtype=jnp.int32)
    matches = owners[:, :, None] == devices[None, None, :]
    inverse = jnp.sum(
        jnp.where(matches, devices[None, :, None], jnp.zeros_like(devices)[None, :, None]), axis=1
    )
    outgoing_keys = jax.vmap(reorder_blocks)(
        kept_keys.reshape(seq_count, seq_devices, block_rows, kv_width), inverse
    )
    outgoing_values = jax.vmap(reorder_blocks)(
        kept_values.reshape(seq_count, seq_devices, block_rows, kv_width), inverse
    )
    incoming = (
        lax.all_to_all(outgoing_keys, "seq", split_axis=1, concat_axis=1, tiled=True),
        lax.all_to_all(outgoing_values, "seq", split_axis=1, concat_axis=1, tiled=True),
    )
    selector = (
        devices[None, :] % slot_span == jnp.arange(slot_span, dtype=jnp.int32)[:, None]
    ).astype(jnp.bfloat16)
    cache_keys = (
        jnp.einsum("md,sdbf->smbf", selector, incoming[0], preferred_element_type=jnp.float32)
        .astype(jnp.bfloat16)
        .reshape(seq_count, slot_span * block_rows, kv_width)
    )
    cache_values = (
        jnp.einsum("md,sdbf->smbf", selector, incoming[1], preferred_element_type=jnp.float32)
        .astype(jnp.bfloat16)
        .reshape(seq_count, slot_span * block_rows, kv_width)
    )
    return (hidden_out, cache_keys, cache_values)


def layer_kernel(
    n, q_hbm, k_hbm, v_hbm, res_hbm, scale_hbm, len_ref, own_hbm, w_ref,
    hid_hbm, ck_hbm, cv_hbm,
    hid_ref, ck_ref, cv_ref, qall, qpart, res_ref, scale_ref, own_ref, kv, other,
    down_out, down_in, pair_out, pair_in, line_out, line_in, skew_out,
    wbuf, acc, den, att, att_out, num_out, num_in, den_out, den_in,
    to_sib, to_x, to_sib2, from_sib, from_x, from_sib2, total, sq_out, sq_in,
    in_sem, w_sem, y_send, y_recv, z_send, z_recv, q_send, q_recv, num_send, num_recv, den_send, den_recv,
    down_send, down_recv, pair_send, pair_recv, line_send, line_recv, skew_send, att_send, att_recv,
    rs_send, rs_recv, sq_send, sq_recv, out_sem,
):
    nz = n // 2
    top = nz - 1
    me = lax.axis_index("seq")
    t = lax.axis_index("tp")
    z, y = me // 2, me % 2
    x, c = t // 2, t % 2
    sib = x * 2 + (1 - c)
    across = (1 - x) * 2 + c
    diagonal = (1 - x) * 2 + (1 - c)
    partner = z * 2 + (1 - y)
    shard = kv.shape[2]
    width = res_ref.shape[1]
    group_cols = qpart.shape[1]
    group = group_cols // HD
    block_rows = shard // n
    chunks = shard // ROWS
    lends = (c == 1) & (z == top)
    hosts = (c == 1) & (z == top - 1)
    takes_kv = (z < top) | (c == 0)
    sends_kv = (z < top - 1) | ((z < top) & (c == 0))

    def half(ref, which, cols):
        return ref.at[:, pl.ds(pl.multiple_of(which * cols, cols), cols)]

    loads = [
        pltpu.make_async_copy(src, dst, in_sem.at[i])
        for i, (src, dst) in enumerate(
            (
                (half(k_hbm, 1 - y, HD), other.at[0]), (half(v_hbm, 1 - y, HD), other.at[1]),
                (half(k_hbm, y, HD), kv.at[me, 0]), (half(v_hbm, y, HD), kv.at[me, 1]),
                (half(q_hbm, 1 - y, group_cols), qpart), (half(q_hbm, y, group_cols), qall.at[y]),
                (own_hbm, own_ref), (res_hbm, res_ref), (scale_hbm, scale_ref),
            )
        )
    ]
    for load in loads[:7]:
        load.start()

    barrier = pltpu.get_barrier_semaphore()
    for peer in (sib, across, diagonal):
        pl.semaphore_signal(barrier, inc=1, device_id={"tp": peer}, device_id_type=MESH)
    for hop in range(1, n):
        pl.semaphore_signal(
            barrier, inc=1, device_id={"seq": lax.rem(me + hop, n)}, device_id_type=MESH
        )

    def clear(s, carry):
        acc[s] = jnp.zeros(acc.shape[1:], jnp.float32)
        den[s] = jnp.zeros(den.shape[1:], jnp.float32)
        return carry

    lax.fori_loop(0, acc.shape[0], clear, 0)
    pl.semaphore_wait(barrier, n + 2)

    def remote(src, dst, send, recv, to):
        return pltpu.make_async_remote_copy(
            src_ref=src, dst_ref=dst, send_sem=send, recv_sem=recv, device_id=to,
            device_id_type=MESH,
        )

    def y_copy(h, origin):
        return remote(
            other.at[h], kv.at[origin, h], y_send.at[h], y_recv.at[h], {"seq": partner}
        )

    def yq_copy(slot):
        return remote(qpart, qall.at[slot], y_send.at[2], y_recv.at[2], {"seq": partner})

    def z_copy(origin, h):
        return remote(
            kv.at[origin, h], kv.at[origin, h], z_send.at[origin, h], z_recv.at[origin, h],
            {"seq": me + 2},
        )

    def lend_copy(yq):
        return remote(
            qall.at[yq], qall.at[2 + yq], q_send.at[yq], q_recv.at[yq], {"seq": me - 2}
        )

    def w_copy(f):
        return pltpu.make_async_copy(
            w_ref.at[:, pl.ds(f * width, width)], wbuf.at[f], w_sem.at[f]
        )

    for h in (0, 1):
        loads[2 + h].wait()
        pl.when(sends_kv)(z_copy(me, h).start)
    for load in (loads[0], loads[1], loads[4], loads[5]):
        load.wait()

    @pl.when(z == top)
    def _():
        yq_copy(y).start()
        for h in (0, 1):
            y_copy(h, me).start()

    @pl.when(z < top)
    def _():
        for h in (0, 1):
            y_copy(h, me).start()
        yq_copy(y).start()

    pl.when(lends)(lend_copy(y).start)
    loads[6].wait()
    for f in range(4):
        w_copy(f).start()
    for load in loads[7:]:
        load.start()

    def owned(device):
        block = own_ref[0, 0] * 0
        for b in range(n):
            block = block + jnp.where(own_ref[0, b] == device, b, 0)
        return jnp.full((block_rows, HD), block, jnp.int32)

    def select(ref, lead, chosen):
        got = jnp.zeros(chosen.shape, jnp.float32)
        for b in range(n):
            rows = ref[(*lead, slice(b * block_rows, (b + 1) * block_rows))]
            got = jnp.where(chosen == b, rows.astype(jnp.float32), got)
        return got.astype(jnp.bfloat16)

    def down_copy(to, slot):
        return remote(
            down_out.at[to], down_in.at[slot], down_send.at[to], down_recv.at[slot], {"seq": to}
        )

    def stage(to, carry):
        chosen = owned(to)
        for h in (0, 1):
            down_out[to, h, y] = select(kv, (me, h), chosen)
            down_out[to, h, 1 - y] = select(other, (h,), chosen)
        return carry

    def post(to, carry):
        down_copy(to, me).start()
        return carry

    lax.fori_loop(0, 2 * z, stage, 0)

    @pl.when(lends)
    def _():
        yq_copy(1 - y).wait_recv()
        lend_copy(1 - y).start()

    for h in (0, 1):
        y_copy(h, partner).wait_recv()
        pl.when(sends_kv)(z_copy(partner, h).start)
    lax.fori_loop(0, 2 * z, post, 0)

    def take(d, j):
        origin = 2 * (z - d) + jnp.where(j == 0, y, 1 - y)
        for h in (0, 1):
            z_copy(origin, h).wait_recv()
            pl.when(sends_kv)(z_copy(origin, h).start)

    @pl.when((z > 0) & takes_kv)
    def _():
        take(1, 0)
        take(1, 1)

    @pl.when(jnp.logical_not(lends))
    def _():
        yq_copy(1 - y).wait_recv()

    def attend(s, origin, masked):
        for hh in range(group):
            slot = s * group + hh
            scores = lax.dot_general(
                qall[s, :, hh * HD : (hh + 1) * HD], kv[origin, 0], (((1,), (1,)), ((), ())),
                preferred_element_type=jnp.float32,
            )
            w = jnp.exp2(jnp.tanh(scores * (HD ** (-0.5) / soft_cap)) * (soft_cap * LOG2E))
            if masked:
                keep = lax.broadcasted_iota(jnp.int32, w.shape, 0) >= lax.broadcasted_iota(
                    jnp.int32, w.shape, 1
                )
                w = jnp.where(keep, w, 0.0)
            folded = w[:, :128]
            for i in range(1, w.shape[1] // 128):
                folded = folded + w[:, i * 128 : (i + 1) * 128]
            den[slot] += folded
            acc[slot] += jnp.dot(
                w.astype(jnp.bfloat16), kv[origin, 1], preferred_element_type=jnp.float32
            )

    def diagonal_block(s, carry):
        attend(s, 2 * z + s, True)
        return carry

    lax.fori_loop(0, 2, diagonal_block, 0)
    attend(1, 2 * z, False)

    @pl.when(hosts)
    def _():
        for yq in (0, 1):
            lend_copy(yq).wait_recv()

        def one(i, carry):
            attend(2 + i // 2, 2 * z + i % 2, False)
            return carry

        lax.fori_loop(0, 4, one, 0)

    def pair_copy(zo):
        return remote(
            pair_out.at[zo], pair_in.at[zo], pair_send.at[zo], pair_recv.at[zo], {"seq": partner}
        )

    def line_copy(zo):
        return remote(
            line_out.at[zo], line_in.at[zo], line_send.at[zo], line_recv.at[zo], {"seq": me + 2}
        )

    def skew_copy(zo):
        return remote(
            skew_out.at[zo], pair_in.at[zo], skew_send.at[zo], pair_recv.at[zo],
            {"seq": partner + 2},
        )

    def gather(zo, device, out):
        chosen = owned(device)
        for yo in (0, 1):
            for h in (0, 1):
                out[zo, yo, h] = select(kv, (2 * zo + yo, h), chosen)

    def pass_cache(zo):
        @pl.when((zo == z) | takes_kv)
        def _():
            gather(zo, partner, pair_out)
            pair_copy(zo).start()

        @pl.when(hosts)
        def _():
            gather(zo, me + 2, line_out)
            line_copy(zo).start()
            gather(zo, partner + 2, skew_out)
            skew_copy(zo).start()

    slots = jnp.where(hosts, 4, 2)

    def phase(d, carry):
        @pl.when(z - d + 1 >= 1)
        def _():
            pass_cache(z - d + 1)

        def side(j, carry):
            @pl.when((z - d >= 0) & takes_kv)
            def _():
                @pl.when(d > 1)
                def _():
                    take(d, j)

                origin = 2 * (z - d) + jnp.where(j == 0, y, 1 - y)

                def one(s, carry):
                    attend(s, origin, False)
                    return carry

                lax.fori_loop(0, slots, one, 0)

            return carry

        lax.fori_loop(0, 2, side, 0)
        return carry

    lax.fori_loop(1, nz, phase, 0)

    def num_copy(yq, r):
        return remote(
            num_out.at[yq, r], num_in.at[yq, r], num_send.at[yq, r], num_recv.at[yq, r],
            {"seq": me + 2},
        )

    def den_copy():
        return remote(den_out, den_in, den_send.at[0], den_recv.at[0], {"seq": me + 2})

    def rows_of(r):
        return pl.ds(pl.multiple_of(r * ROWS, ROWS), ROWS)

    @pl.when(hosts)
    def _():
        for s in range(2 * group):
            for r in range(chunks):
                cols = slice(r * ROWS, (r + 1) * ROWS)
                line = jnp.sum(den[2 * group + s, cols, :].T, axis=0, keepdims=True)
                den_out[s, :, cols] = jnp.broadcast_to(line, (8, ROWS))
        den_copy().start()

        def give(i, carry):
            yq = jnp.where(i < chunks, 1 - y, y)
            r = i % chunks
            for hh in range(group):
                num_out[yq, r, :, hh * HD : (hh + 1) * HD] = acc[
                    (2 + yq) * group + hh, rows_of(r), :
                ].astype(jnp.bfloat16)
            num_copy(yq, r).start()
            return carry

        lax.fori_loop(0, 2 * chunks, give, 0)

    def att_copy(r, g):
        return remote(
            att_out.at[r], att.at[g, r], att_send.at[r], att_recv.at[r], {"seq": partner}
        )

    pl.when(lends)(den_copy().wait_recv)

    def finish(yq, r, put):
        rows = rows_of(r)

        @pl.when(lends)
        def _():
            num_copy(yq, r).wait_recv()
            for hh in range(group):
                slot = yq * group + hh
                acc[slot, rows, :] += num_in[yq, r, :, hh * HD : (hh + 1) * HD].astype(jnp.float32)
                line = den_in[slot, :1, rows]
                spread = jnp.broadcast_to(line, (128, ROWS)).T
                first = lax.broadcasted_iota(jnp.int32, spread.shape, 1) == 0
                den[slot, rows, :] += jnp.where(first, spread, 0.0)

        for hh in range(group):
            slot = yq * group + hh
            put(
                hh,
                (
                    acc[slot, rows, :] / jnp.sum(den[slot, rows, :], axis=-1, keepdims=True)
                ).astype(jnp.bfloat16),
            )

    def away(r, carry):
        def put(hh, value):
            att_out[r, :, hh * HD : (hh + 1) * HD] = value

        finish(1 - y, r, put)
        att_copy(r, y).start()
        return carry

    def home(r, carry):
        def put(hh, value):
            att[y, r, :, hh * HD : (hh + 1) * HD] = value

        finish(y, r, put)
        return carry

    lax.fori_loop(0, chunks, away, 0)
    lax.fori_loop(0, chunks, home, 0)

    def rs_copy(kind, r, src, dst, to):
        return remote(
            src.at[r], dst.at[r], rs_send.at[kind, r], rs_recv.at[kind, r], {"tp": to}
        )

    def sib_copy(r):
        return rs_copy(0, r, to_sib, from_sib, sib)

    def x_copy(r):
        return rs_copy(1, r, to_x, from_x, across)

    def sib2_copy(r):
        return rs_copy(2, r, to_sib2, from_sib2, sib)

    def part(f, r):
        return jnp.dot(
            att[0, r], wbuf[f, :group_cols, :], preferred_element_type=jnp.float32
        ) + jnp.dot(att[1, r], wbuf[f, group_cols:, :], preferred_element_type=jnp.float32)

    for f in range(4):
        w_copy(f).wait()

    def first(r, carry):
        att_copy(r, 1 - y).wait_recv()
        to_sib[r] = part(diagonal, r).astype(jnp.bfloat16)
        sib_copy(r).start()
        return carry

    def second(r, carry):
        mine = part(across, r)
        sib_copy(r).wait_recv()
        to_x[r] = (mine + from_sib[r].astype(jnp.float32)).astype(jnp.bfloat16)
        x_copy(r).start()
        return carry

    def third(r, carry):
        to_sib2[r] = part(sib, r).astype(jnp.bfloat16)
        sib2_copy(r).start()
        return carry

    def fourth(r, carry):
        total[r] = part(t, r)
        return carry

    for step in (first, second):
        lax.fori_loop(0, chunks, step, 0)

    pass_cache(0)

    for step in (third, fourth):
        lax.fori_loop(0, chunks, step, 0)

    mine_blocks = owned(me)
    local_row = lax.broadcasted_iota(jnp.int32, mine_blocks.shape, 0)
    bound = jnp.full(mine_blocks.shape, len_ref[0], jnp.int32)

    def cache(zo, carry):
        far = lends & (zo < top)

        @pl.when(zo <= z)
        def _():
            skew_copy(zo).wait_recv()

        @pl.when(far)
        def _():
            line_copy(zo).wait_recv()

        for yo in (0, 1):
            origin = 2 * zo + yo
            pos = local_row + mine_blocks * block_rows + origin * shard
            live = (pos < bound) & (pos >= bound - WINDOW)
            rows = pl.ds(pl.multiple_of(origin * block_rows, block_rows), block_rows)

            @pl.when(zo > z)
            def _():
                down_copy(origin, origin).wait_recv()

            for h, out in enumerate((ck_ref, cv_ref)):

                def put(g, value):
                    cols = pl.ds(pl.multiple_of(g * HD, HD), HD)
                    out[rows, cols] = jnp.where(live, value.astype(jnp.float32), 0.0).astype(
                        jnp.bfloat16
                    )

                @pl.when(zo > z)
                def _():
                    for g in (0, 1):
                        put(g, down_in[origin, h, g])

                @pl.when(zo <= z)
                def _():
                    put(1 - y, pair_in[zo, yo, h])

                @pl.when((zo <= z) & jnp.logical_not(far))
                def _():
                    put(y, select(kv, (origin, h), mine_blocks))

                @pl.when(far)
                def _():
                    put(y, line_in[zo, yo, h])

        return carry

    lax.fori_loop(0, nz, cache, 0)
    rest = ck_ref.shape[0] - n * block_rows
    if rest:
        for out in (ck_ref, cv_ref):
            out[n * block_rows :, :] = jnp.zeros((rest, 2 * HD), jnp.bfloat16)
    outs = [
        pltpu.make_async_copy(src, dst, out_sem.at[i])
        for i, (src, dst) in enumerate(((ck_ref, ck_hbm), (cv_ref, cv_hbm), (hid_ref, hid_hbm)))
    ]
    outs[0].start()
    outs[1].start()

    for r in range(chunks):
        sib2_copy(r).wait_recv()
        x_copy(r).wait_recv()
        branch = total[r] + from_sib2[r].astype(jnp.float32) + from_x[r].astype(jnp.float32)
        total[r] = branch
        squared = branch * branch
        folded = squared[:, :128]
        for i in range(1, squared.shape[1] // 128):
            folded = folded + squared[:, i * 128 : (i + 1) * 128]
        line = jnp.sum(folded.T, axis=0, keepdims=True)
        sq_out[:, r * ROWS : (r + 1) * ROWS] = jnp.broadcast_to(line, (8, ROWS))

    def sq_copy(i, to, slot):
        return pltpu.make_async_remote_copy(
            src_ref=sq_out, dst_ref=sq_in.at[slot], send_sem=sq_send.at[i],
            recv_sem=sq_recv.at[slot], device_id={"tp": to}, device_id_type=MESH,
        )

    peers = (sib, across, diagonal)
    for i, peer in enumerate(peers):
        sq_copy(i, peer, t).start()
    squares = sq_out[...]
    for i, peer in enumerate(peers):
        sq_copy(i, peer, peer).wait_recv()
        squares = squares + sq_in[peer]
    loads[7].wait()
    loads[8].wait()
    factor = lax.rsqrt(squares / D + norm_eps)
    for r in range(chunks):
        line = jnp.broadcast_to(factor[:1, r * ROWS : (r + 1) * ROWS], (128, ROWS))
        spread = line.T
        for i in range(res_ref.shape[1] // 128):
            cols = slice(i * 128, (i + 1) * 128)
            rows = slice(r * ROWS, (r + 1) * ROWS)
            normed = total[r, :, cols] * spread * scale_ref[cols].reshape(1, 128)
            hid_ref[rows, cols] = (res_ref[rows, cols].astype(jnp.float32) + normed).astype(
                jnp.bfloat16
            )

    outs[2].start()
    for i, peer in enumerate(peers):
        sq_copy(i, peer, t).wait_send()
    for r in range(chunks):
        sib_copy(r).wait_send()
        x_copy(r).wait_send()
        sib2_copy(r).wait_send()

    for h in (0, 1):
        y_copy(h, me).wait_send()
    yq_copy(y).wait_send()
    for r in range(chunks):
        att_copy(r, y).wait_send()

    def settle_kv(origin, carry):
        for h in (0, 1):
            z_copy(origin, h).wait_send()
        return carry

    @pl.when(sends_kv)
    def _():
        lax.fori_loop(0, 2 * z + 2, settle_kv, 0)

    @pl.when(lends)
    def _():
        for yq in (0, 1):
            lend_copy(yq).wait_send()

    @pl.when(hosts)
    def _():
        den_copy().wait_send()
        for yq in (0, 1):
            for r in range(chunks):
                num_copy(yq, r).wait_send()

    def settle(to, carry):
        down_copy(to, me).wait_send()
        return carry

    lax.fori_loop(0, 2 * z, settle, 0)

    def settle_cache(zo, carry):
        @pl.when((zo == z) | takes_kv)
        def _():
            pair_copy(zo).wait_send()

        @pl.when(hosts)
        def _():
            line_copy(zo).wait_send()
            skew_copy(zo).wait_send()

        return carry

    lax.fori_loop(0, z + 1, settle_cache, 0)
    for out in outs:
        out.wait()


def put_out(*refs):
    count = (len(refs) - 1) // 3
    sems = refs[-1]
    copies = [
        (
            pltpu.make_async_copy(refs[i], refs[2 * count + i], sems.at[0, i]),
            pltpu.make_async_copy(refs[2 * count + i], refs[count + i], sems.at[1, i]),
        )
        for i in range(count)
    ]
    for read, _ in copies:
        read.start()
    for read, write in copies:
        read.wait()
        write.start()
    for _, write in copies:
        write.wait()


def fused(n, queries, key_rows, value_rows, residual, out_weight, post_scale, lengths, owners):
    shard, q_width = queries.shape[1:]
    kv_width = key_rows.shape[2]
    width = residual.shape[2]
    heads = q_width // HD
    chunks = shard // ROWS
    cache_rows = WINDOW // n
    smem = pl.BlockSpec(memory_space=pltpu.SMEM)
    apart = pl.BlockSpec(memory_space=pl.ANY)
    group_cols = q_width * HD // kv_width
    slab = pltpu.VMEM((n // 2, 2, 2, shard // n, HD), jnp.bfloat16)
    half = pltpu.VMEM((chunks, ROWS, width), jnp.bfloat16)
    hidden, ck, cv = pl.pallas_call(
        functools.partial(layer_kernel, n),
        out_shape=(
            jax.ShapeDtypeStruct((shard, width), jnp.bfloat16),
            jax.ShapeDtypeStruct((cache_rows, kv_width), jnp.bfloat16),
            jax.ShapeDtypeStruct((cache_rows, kv_width), jnp.bfloat16),
        ),
        in_specs=[apart] * 5 + [smem] + [apart] * 2,
        out_specs=(apart,) * 3,
        scratch_shapes=[
            pltpu.VMEM((shard, width), jnp.bfloat16),
            pltpu.VMEM((cache_rows, kv_width), jnp.bfloat16),
            pltpu.VMEM((cache_rows, kv_width), jnp.bfloat16),
            pltpu.VMEM((4, shard, group_cols), jnp.bfloat16),
            pltpu.VMEM((shard, group_cols), jnp.bfloat16),
            pltpu.VMEM((shard, width), jnp.bfloat16),
            pltpu.VMEM((width,), jnp.float32),
            pltpu.SMEM((1, n), jnp.int32),
            pltpu.VMEM((n, 2, shard, HD), jnp.bfloat16),
            pltpu.VMEM((2, shard, HD), jnp.bfloat16),
            pltpu.VMEM((n, 2, 2, shard // n, HD), jnp.bfloat16),
            pltpu.VMEM((n, 2, 2, shard // n, HD), jnp.bfloat16),
            slab, slab, slab, slab, slab,
            pltpu.VMEM((4, q_width, width), jnp.bfloat16),
            pltpu.VMEM((2 * heads, shard, HD), jnp.float32),
            pltpu.VMEM((2 * heads, shard, 128), jnp.float32),
            pltpu.VMEM((2, chunks, ROWS, group_cols), jnp.bfloat16),
            pltpu.VMEM((chunks, ROWS, group_cols), jnp.bfloat16),
            pltpu.VMEM((2, chunks, ROWS, group_cols), jnp.bfloat16),
            pltpu.VMEM((2, chunks, ROWS, group_cols), jnp.bfloat16),
            pltpu.VMEM((heads, 8, shard), jnp.float32),
            pltpu.VMEM((heads, 8, shard), jnp.float32),
            half, half, half, half, half, half,
            pltpu.VMEM((chunks, ROWS, width), jnp.float32),
            pltpu.VMEM((8, shard), jnp.float32),
            pltpu.VMEM((4, 8, shard), jnp.float32),
            pltpu.SemaphoreType.DMA((9,)),
            pltpu.SemaphoreType.DMA((4,)),
            pltpu.SemaphoreType.DMA((3,)),
            pltpu.SemaphoreType.DMA((3,)),
            pltpu.SemaphoreType.DMA((n, 2)),
            pltpu.SemaphoreType.DMA((n, 2)),
            pltpu.SemaphoreType.DMA((2,)),
            pltpu.SemaphoreType.DMA((2,)),
            pltpu.SemaphoreType.DMA((2, chunks)),
            pltpu.SemaphoreType.DMA((2, chunks)),
            pltpu.SemaphoreType.DMA((1,)),
            pltpu.SemaphoreType.DMA((1,)),
            pltpu.SemaphoreType.DMA((n,)),
            pltpu.SemaphoreType.DMA((n,)),
            pltpu.SemaphoreType.DMA((n // 2,)),
            pltpu.SemaphoreType.DMA((n // 2,)),
            pltpu.SemaphoreType.DMA((n // 2,)),
            pltpu.SemaphoreType.DMA((n // 2,)),
            pltpu.SemaphoreType.DMA((n // 2,)),
            pltpu.SemaphoreType.DMA((chunks,)),
            pltpu.SemaphoreType.DMA((chunks,)),
            pltpu.SemaphoreType.DMA((3, chunks)),
            pltpu.SemaphoreType.DMA((3, chunks)),
            pltpu.SemaphoreType.DMA((3,)),
            pltpu.SemaphoreType.DMA((4,)),
            pltpu.SemaphoreType.DMA((3,)),
        ],
        compiler_params=pltpu.CompilerParams(
            collective_id=0, has_side_effects=True, vmem_limit_bytes=60 * 1024 * 1024
        ),
    )(
        queries[0], key_rows[0], value_rows[0], residual[0], post_scale, lengths, owners,
        out_weight,
    )
    made = (hidden, ck, cv)
    hidden, ck, cv = pl.pallas_call(
        put_out,
        out_shape=tuple(jax.ShapeDtypeStruct(a.shape, a.dtype) for a in made),
        in_specs=[apart] * len(made),
        out_specs=(apart,) * len(made),
        scratch_shapes=[pltpu.VMEM(a.shape, a.dtype) for a in made]
        + [pltpu.SemaphoreType.DMA((2, len(made)))],
    )(*made)
    return hidden[None], ck[None], cv[None]


def solution(mesh):
    placed = (
        P(None, "seq", "tp"),
        P(None, "seq", "tp"),
        P(None, "seq", "tp"),
        P(None, "seq", "tp"),
        P("tp", None),
        P("tp"),
        P(),
        P(),
    )
    return jax.shard_map(
        local,
        mesh=mesh,
        in_specs=placed,
        out_specs=(P(None, "seq", "tp"), P(None, "seq", "tp"), P(None, "seq", "tp")),
        check_vma=False,
    )
```

```python
import functools

import jax
import jax.numpy as jnp
from jax import lax
from jax.experimental import pallas as pl
from jax.experimental.pallas import tpu as pltpu
from jax.sharding import PartitionSpec as P

D = 3584
HD = 256
WINDOW = 4096
MESH = pl.DeviceIdType.MESH
LOG2E = 1.4426950408889634
ROWS = 64
LANES = 128


soft_cap = 50.0
norm_eps = 1e-06


def shifted(x, axis, by):
    peers = lax.axis_size(axis)
    pairs = [(i, i + by) for i in range(peers) if 0 <= i + by < peers]
    return lax.ppermute(x, axis, pairs)


def attend_block(grouped, block_keys, block_values, query_pos, key_pos, state_pair):
    numerator, denominator = state_pair
    seq_count, query_count, kv_local, group_size, head_size = grouped.shape
    keyed_rows = block_keys.reshape(seq_count, block_keys.shape[1], kv_local, head_size)
    valued_rows = block_values.reshape(seq_count, block_values.shape[1], kv_local, head_size)
    scores = jnp.einsum(
        "sqhgd,skhd->shgqk", grouped, keyed_rows, preferred_element_type=jnp.float32
    ) * head_size ** (-0.5)
    capped = soft_cap * jnp.tanh(scores / soft_cap)
    spread = query_pos[:, None] - key_pos[None, :]
    live_mask = (spread >= 0) & (spread < WINDOW) & (key_pos[None, :] >= 0)
    weights = jnp.where(live_mask, jnp.exp(capped), jnp.zeros_like(capped))
    denominator = denominator + jnp.sum(weights, axis=-1)
    numerator = numerator + jnp.einsum(
        "shgqk,skhd->sqhgd",
        weights.astype(jnp.bfloat16),
        valued_rows,
        preferred_element_type=jnp.float32,
    )
    return (numerator, denominator)


def reorder_blocks(blocked, ordering):
    return blocked[ordering]


def local(queries, key_rows, value_rows, residual, out_weight, post_scale, lengths, owners):
    seq_count, shard_len, query_width = queries.shape
    seq_size = lax.axis_size("seq")
    if (
        seq_count == 1 and lax.axis_size("tp") == 4 and seq_size % 2 == 0 and seq_size >= 6
        and seq_size * shard_len <= WINDOW and key_rows.shape[2] == 2 * HD
        and shard_len % LANES == 0
    ):
        return fused(
            seq_size, queries, key_rows, value_rows, residual, out_weight, post_scale, lengths,
            owners,
        )
    kv_width = key_rows.shape[2]
    kv_local = kv_width // HD
    group_size = query_width // kv_width
    grouped = queries.reshape(seq_count, shard_len, kv_local, group_size, HD)
    position = lax.axis_index("seq")
    seq_devices = lax.axis_size("seq")
    offsets = jnp.arange(shard_len, dtype=jnp.int32)
    query_pos = position * shard_len + offsets
    numerator = jnp.zeros((seq_count, shard_len, kv_local, group_size, HD), jnp.float32)
    denominator = jnp.zeros((seq_count, kv_local, group_size, shard_len), jnp.float32)
    state_pair = attend_block(
        grouped, key_rows, value_rows, query_pos, query_pos, (numerator, denominator)
    )
    hop_count = min(WINDOW // shard_len, seq_devices - 1)
    arrived = []
    current = (key_rows, value_rows)
    for hop_index in range(1, hop_count + 1):
        current = shifted((current[0], current[1]), "seq", 1)
        arrived.append((hop_index, current))
        if len(arrived) == 2 or hop_index == hop_count:
            ordered = arrived[::-1]
            block_keys = jnp.concatenate([member[1][0] for member in ordered], axis=1)
            block_values = jnp.concatenate([member[1][1] for member in ordered], axis=1)
            block_pos = jnp.concatenate(
                [(position - member[0]) * shard_len + offsets for member in ordered]
            )
            state_pair = attend_block(
                grouped, block_keys, block_values, query_pos, block_pos, state_pair
            )
            arrived = []
    numerator, denominator = state_pair
    attended = (numerator / jnp.transpose(denominator, (0, 3, 1, 2))[..., None]).astype(
        jnp.bfloat16
    )
    partial_value = jnp.dot(
        attended.reshape(seq_count * shard_len, query_width),
        out_weight,
        preferred_element_type=jnp.float32,
    )
    partial_value = partial_value.reshape(seq_count, shard_len, out_weight.shape[1])
    branch = lax.psum_scatter(partial_value, "tp", scatter_dimension=2, tiled=True)
    squares = lax.psum(jnp.sum(branch * branch, axis=-1), "tp")
    normed = branch * lax.rsqrt(squares / D + norm_eps)[..., None] * post_scale
    hidden_out = (residual.astype(jnp.float32) + normed).astype(jnp.bfloat16)
    block_rows = shard_len // seq_devices
    slot_span = WINDOW // shard_len
    live_rows = (query_pos[None, :] >= lengths[:, None] - WINDOW) & (
        query_pos[None, :] < lengths[:, None]
    )
    kept_keys = jnp.where(live_rows[..., None], key_rows, jnp.zeros_like(key_rows))
    kept_values = jnp.where(live_rows[..., None], value_rows, jnp.zeros_like(value_rows))
    devices = jnp.arange(seq_devices, dtype=jnp.int32)
    matches = owners[:, :, None] == devices[None, None, :]
    inverse = jnp.sum(
        jnp.where(matches, devices[None, :, None], jnp.zeros_like(devices)[None, :, None]), axis=1
    )
    outgoing_keys = jax.vmap(reorder_blocks)(
        kept_keys.reshape(seq_count, seq_devices, block_rows, kv_width), inverse
    )
    outgoing_values = jax.vmap(reorder_blocks)(
        kept_values.reshape(seq_count, seq_devices, block_rows, kv_width), inverse
    )
    incoming = (
        lax.all_to_all(outgoing_keys, "seq", split_axis=1, concat_axis=1, tiled=True),
        lax.all_to_all(outgoing_values, "seq", split_axis=1, concat_axis=1, tiled=True),
    )
    selector = (
        devices[None, :] % slot_span == jnp.arange(slot_span, dtype=jnp.int32)[:, None]
    ).astype(jnp.bfloat16)
    cache_keys = (
        jnp.einsum("md,sdbf->smbf", selector, incoming[0], preferred_element_type=jnp.float32)
        .astype(jnp.bfloat16)
        .reshape(seq_count, slot_span * block_rows, kv_width)
    )
    cache_values = (
        jnp.einsum("md,sdbf->smbf", selector, incoming[1], preferred_element_type=jnp.float32)
        .astype(jnp.bfloat16)
        .reshape(seq_count, slot_span * block_rows, kv_width)
    )
    return (hidden_out, cache_keys, cache_values)


def layer_kernel(
    n, q_hbm, k_hbm, v_hbm, res_hbm, scale_hbm, len_ref, own_hbm, w_ref,
    hid_ref, ck_ref, cv_ref,
    qall, qpart, res_ref, scale_ref, own_ref, kv, other,
    down_out, down_in, pair_out, pair_in, line_out, line_in, skew_out,
    wbuf, acc, den, att, att_out, lent_out,
    to_sib, to_x, to_sib2, from_sib, from_x, from_sib2, early, total, folds, sq_out, sq_in,
    in_sem, w_sem, y_send, yq_send, y_recv, z_send, z_recv, lend_recv, q_send, q_recv, lent_send,
    down_send, down_recv, pair_send, pair_recv, line_send, line_recv, skew_send, att_send, att_recv,
    rs_send, rs_recv, sib2_recv, sq_send, sq_recv,
):
    nz = n // 2
    top = nz - 1
    me = lax.axis_index("seq")
    t = lax.axis_index("tp")
    z, y = me // 2, me % 2
    x, c = t // 2, t % 2
    sib = x * 2 + (1 - c)
    across = (1 - x) * 2 + c
    diagonal = (1 - x) * 2 + (1 - c)
    partner = z * 2 + (1 - y)
    shard = kv.shape[2]
    width = res_ref.shape[1]
    group_cols = qpart.shape[1]
    group = group_cols // HD
    block_rows = shard // n
    chunks = shard // ROWS
    lends = (c == 1) & (z == top)
    hosts = (c == 1) & (z == top - 1)
    takes_kv = (z < top) | (c == 0)
    sends_kv = (z < top - 1) | ((z < top) & (c == 0))

    def half(ref, which, cols):
        return ref.at[:, pl.ds(pl.multiple_of(which * cols, cols), cols)]

    loads = [
        pltpu.make_async_copy(src, dst, in_sem.at[i])
        for i, (src, dst) in enumerate(
            (
                (half(k_hbm, 1 - y, HD), other.at[0]), (half(v_hbm, 1 - y, HD), other.at[1]),
                (half(k_hbm, y, HD), kv.at[me, 0]), (half(v_hbm, y, HD), kv.at[me, 1]),
                (half(q_hbm, 1 - y, group_cols), qpart), (half(q_hbm, y, group_cols), qall.at[y]),
                (own_hbm, own_ref), (res_hbm, res_ref), (scale_hbm, scale_ref),
            )
        )
    ]
    for load in loads[:7]:
        load.start()

    barrier = pltpu.get_barrier_semaphore()
    for peer in (sib, across, diagonal):
        pl.semaphore_signal(barrier, inc=1, device_id={"tp": peer}, device_id_type=MESH)
    for hop in range(1, n):
        pl.semaphore_signal(
            barrier, inc=1, device_id={"seq": lax.rem(me + hop, n)}, device_id_type=MESH
        )

    def clear(s, carry):
        acc[s] = jnp.zeros(acc.shape[1:], jnp.float32)
        den[s] = jnp.zeros(den.shape[1:], jnp.float32)
        return carry

    lax.fori_loop(0, acc.shape[0], clear, 0)
    pl.semaphore_wait(barrier, n + 2)

    def remote(src, dst, send, recv, to):
        return pltpu.make_async_remote_copy(
            src_ref=src, dst_ref=dst, send_sem=send, recv_sem=recv, device_id=to,
            device_id_type=MESH,
        )

    def settle(ref, sem):
        pltpu.make_async_copy(ref, ref, sem.at[0]).wait()

    def y_copy(h, origin):
        return remote(
            other.at[h], kv.at[origin, h], y_send.at[0], y_recv.at[h], {"seq": partner}
        )

    def yq_copy(slot):
        return remote(qpart, qall.at[slot], yq_send.at[0], y_recv.at[2], {"seq": partner})

    def z_copy(origin, h):
        return remote(
            kv.at[origin, h], kv.at[origin, h], z_send.at[0], z_recv.at[origin, h],
            {"seq": me + 2},
        )

    def lend_copy(yq):
        return remote(
            qall.at[yq], qall.at[2 + yq], q_send.at[0], q_recv.at[0], {"seq": me - 2}
        )

    def lend_kv(origin, h):
        return remote(
            kv.at[origin, h], kv.at[origin, h], z_send.at[0], lend_recv.at[0],
            {"seq": me - 2},
        )

    def w_copy(f, g):
        return pltpu.make_async_copy(
            w_ref.at[pl.ds(g * group_cols, group_cols), pl.ds(f * width, width)],
            wbuf.at[f, g], w_sem.at[0],
        )

    for h in (0, 1):
        loads[2 + h].wait()
        pl.when(sends_kv)(z_copy(me, h).start)
    for load in (loads[0], loads[1], loads[4], loads[5]):
        load.wait()

    @pl.when(z == top)
    def _():
        yq_copy(y).start()
        for h in (0, 1):
            y_copy(h, me).start()

    @pl.when(z < top)
    def _():
        for h in (0, 1):
            y_copy(h, me).start()
        yq_copy(y).start()

    @pl.when(lends)
    def _():
        lend_copy(y).start()
        for h in (0, 1):
            lend_kv(me, h).start()

    loads[6].wait()
    for f in range(4):
        for g in (0, 1):
            w_copy(f, g).start()
    for load in loads[7:]:
        load.start()

    def owned(device):
        block = own_ref[0, 0] * 0
        for b in range(n):
            block = block + jnp.where(own_ref[0, b] == device, b, 0)
        return jnp.full((block_rows, HD), block, jnp.int32)

    def select(ref, lead, chosen):
        got = jnp.zeros(chosen.shape, jnp.float32)
        for b in range(n):
            rows = ref[(*lead, slice(b * block_rows, (b + 1) * block_rows))]
            got = jnp.where(chosen == b, rows.astype(jnp.float32), got)
        return got.astype(jnp.bfloat16)

    def down_copy(to, slot):
        return remote(
            down_out.at[to], down_in.at[slot], down_send.at[0], down_recv.at[0], {"seq": to}
        )

    def stage(to, carry):
        chosen = owned(to)
        for h in (0, 1):
            down_out[to, h, y] = select(kv, (me, h), chosen)
            down_out[to, h, 1 - y] = select(other, (h,), chosen)
        return carry

    def post(to, carry):
        down_copy(to, me).start()
        return carry

    lax.fori_loop(0, 2 * z, stage, 0)

    @pl.when(lends)
    def _():
        yq_copy(1 - y).wait_recv()
        lend_copy(1 - y).start()

    for h in (0, 1):
        y_copy(h, partner).wait_recv()
        pl.when(sends_kv)(z_copy(partner, h).start)
        pl.when(lends)(lend_kv(partner, h).start)
    lax.fori_loop(0, 2 * z, post, 0)

    def take(d, j):
        origin = 2 * (z - d) + jnp.where(j == 0, y, 1 - y)
        for h in (0, 1):
            z_copy(origin, h).wait_recv()
            pl.when(sends_kv)(z_copy(origin, h).start)

    @pl.when((z > 0) & takes_kv)
    def _():
        take(1, 0)
        take(1, 1)

    @pl.when(jnp.logical_not(lends))
    def _():
        yq_copy(1 - y).wait_recv()

    def attend(base, origin, above):
        pair = pl.ds(base, 2)
        for hh in range(group):
            stacked = qall[pair, :, hh * HD : (hh + 1) * HD].reshape(2 * shard, HD)
            scores = lax.dot_general(
                stacked, kv[origin, 0], (((1,), (1,)), ((), ())),
                preferred_element_type=jnp.float32,
            )
            w = jnp.exp2(jnp.tanh(scores * (HD ** (-0.5) / soft_cap)) * (soft_cap * LOG2E))
            if above is not None:
                keep = lax.broadcasted_iota(jnp.int32, w.shape, 0) >= above + (
                    lax.broadcasted_iota(jnp.int32, w.shape, 1)
                )
                w = jnp.where(keep, w, 0.0)
            folded = w[:, :LANES]
            for i in range(1, w.shape[1] // LANES):
                folded = folded + w[:, i * LANES : (i + 1) * LANES]
            den[hh, pair] += folded.reshape(2, shard, LANES)
            acc[hh, pair] += jnp.dot(
                w.astype(jnp.bfloat16), kv[origin, 1], preferred_element_type=jnp.float32
            ).reshape(2, shard, HD)

    def own_slab(base, slab):
        def diagonal_block(i, carry):
            attend(base, 2 * slab + i, i * shard)
            return carry

        lax.fori_loop(0, 2, diagonal_block, 0)

    pl.when(jnp.logical_not(lends))(functools.partial(own_slab, 0, z))
    @pl.when(hosts)
    def _():
        settle(qall.at[2:], q_recv)

        def one(i, carry):
            attend(2, 2 * z + i, None)
            return carry

        lax.fori_loop(0, 2, one, 0)

    def pair_copy(zo):
        return remote(
            pair_out.at[zo], pair_in.at[zo], pair_send.at[0], pair_recv.at[0], {"seq": partner}
        )

    def line_copy(zo):
        return remote(
            line_out.at[zo], line_in.at[zo], line_send.at[0], line_recv.at[0], {"seq": me + 2}
        )

    def skew_copy(zo):
        return remote(
            skew_out.at[zo], pair_in.at[zo], skew_send.at[0], pair_recv.at[0],
            {"seq": partner + 2},
        )

    def gather(zo, device, out):
        chosen = owned(device)
        for yo in (0, 1):
            for h in (0, 1):
                out[zo, yo, h] = select(kv, (2 * zo + yo, h), chosen)

    def pass_cache(zo):
        @pl.when((zo == z) | takes_kv)
        def _():
            gather(zo, partner, pair_out)
            pair_copy(zo).start()

        @pl.when(hosts)
        def _():
            gather(zo, me + 2, line_out)
            line_copy(zo).start()
            gather(zo, partner + 2, skew_out)
            skew_copy(zo).start()

    pairs = jnp.where(hosts, 2, 1)

    def phase(d, carry):
        @pl.when(z - d + 1 >= 1)
        def _():
            pass_cache(z - d + 1)

        @pl.when(hosts & (d == jnp.minimum(2, z)))
        def _():
            settle(kv.at[2 * top :], lend_recv)
            own_slab(2, top)

        def side(j, carry):
            @pl.when((z - d >= 0) & takes_kv)
            def _():
                @pl.when(d > 1)
                def _():
                    take(d, j)

                origin = 2 * (z - d) + jnp.where(j == 0, y, 1 - y)

                def one(i, carry):
                    attend(2 * i, origin, None)
                    return carry

                lax.fori_loop(0, pairs, one, 0)

            return carry

        lax.fori_loop(0, 2, side, 0)
        return carry

    lax.fori_loop(1, nz, phase, 0)

    def rows_of(r):
        return pl.ds(pl.multiple_of(r * ROWS, ROWS), ROWS)

    def att_copy(r, g):
        return remote(
            att_out.at[r], att.at[g, r], att_send.at[0], att_recv.at[r], {"seq": partner}
        )

    def lent_copy(yq, r, g):
        return remote(
            lent_out.at[yq, r], att.at[g, r], lent_send.at[0], att_recv.at[r],
            {"seq": 2 * top + yq},
        )

    def finish(s, r, out, lead):
        for hh in range(group):
            out[(*lead, slice(None), slice(hh * HD, (hh + 1) * HD))] = (
                acc[hh, s, rows_of(r), :]
                / jnp.sum(den[hh, s, rows_of(r), :], axis=-1, keepdims=True)
            ).astype(jnp.bfloat16)

    def away(r, carry):
        finish(1 - y, r, att_out, (r,))
        att_copy(r, y).start()
        return carry

    def home(r, carry):
        finish(y, r, att, (y, r))
        return carry

    def give(r, carry):
        for yq in (1 - y, y):
            finish(2 + yq, r, lent_out, (yq, r))
            lent_copy(yq, r, y).start()
        return carry

    @pl.when(jnp.logical_not(lends))
    def _():
        lax.fori_loop(0, chunks, away, 0)
        lax.fori_loop(0, chunks, home, 0)

    def rs_copy(kind, r, src, dst, recv, to):
        return remote(src.at[r], dst.at[r], rs_send.at[kind], recv, {"tp": to})

    def sib_copy(r):
        return rs_copy(0, r, to_sib, from_sib, rs_recv.at[0, r], sib)

    def x_copy(r):
        return rs_copy(1, r, to_x, from_x, rs_recv.at[1, r], across)

    def sib2_copy(r):
        return rs_copy(2, r, to_sib2, from_sib2, sib2_recv.at[0], sib)

    def product(rows, f, g):
        return jnp.dot(rows, wbuf[f, g], preferred_element_type=jnp.float32)

    def part(f, r):
        pair = pl.ds(2 * r, 2)
        rows = [att[g, pair].reshape(2 * ROWS, group_cols) for g in (0, 1)]
        return product(rows[0], f, 0) + product(rows[1], f, 1)

    settle(wbuf, w_sem)

    sent = (diagonal, across)

    @pl.when(jnp.logical_not(lends))
    def _():
        for i, f in enumerate(sent):
            early[i] = product(att[y].reshape(shard, group_cols), f, y)

    @pl.when(hosts)
    def _():
        lax.fori_loop(0, chunks, give, 0)

    def send_sib(r):
        pl.when(jnp.logical_not(lends))(att_copy(r, 1 - y).wait_recv)

        @pl.when(lends)
        def _():
            both_heads = att.at[:, r]
            pltpu.make_async_copy(both_heads, both_heads, att_recv.at[r]).wait()
            for i, f in enumerate(sent):
                early[i, rows_of(r), :] = product(att[y, r], f, y)

        to_sib[r] = (early[0, rows_of(r), :] + product(att[1 - y, r], diagonal, 1 - y)).astype(
            jnp.bfloat16
        )
        sib_copy(r).start()

    def send_x(r):
        mine = early[1, rows_of(r), :] + product(att[1 - y, r], across, 1 - y)
        sib_copy(r).wait_recv()
        to_x[r] = (mine + from_sib[r].astype(jnp.float32)).astype(jnp.bfloat16)
        x_copy(r).start()

    def both(r, carry):
        pl.when(r < chunks)(functools.partial(send_sib, r))
        pl.when(r > 0)(functools.partial(send_x, r - 1))
        return carry

    def third(r, carry):
        pair = pl.ds(2 * r, 2)
        to_sib2[pair] = part(sib, r).astype(jnp.bfloat16).reshape(2, ROWS, width)
        for i in (0, 1):
            sib2_copy(2 * r + i).start()
        return carry

    def fourth(r, carry):
        rows = pl.ds(pl.multiple_of(2 * r * ROWS, 2 * ROWS), 2 * ROWS)
        total[rows, :] = part(t, r)
        return carry

    lax.fori_loop(0, chunks + 1, both, 0)

    pass_cache(0)

    for step in (third, fourth):
        lax.fori_loop(0, chunks // 2, step, 0)

    mine_blocks = owned(me)
    local_row = lax.broadcasted_iota(jnp.int32, mine_blocks.shape, 0)
    bound = jnp.full(mine_blocks.shape, len_ref[0], jnp.int32)

    for slab in range(nz):

        @pl.when(z == slab)
        def _():
            settle(pair_in.at[: slab + 1], pair_recv)
            if slab < top:
                settle(down_in.at[2 * slab + 2 :], down_recv)

    @pl.when(lends)
    def _():
        settle(line_in.at[:top], line_recv)

    def cache(zo, carry):
        far = lends & (zo < top)

        for yo in (0, 1):
            origin = 2 * zo + yo
            pos = local_row + mine_blocks * block_rows + origin * shard
            live = (pos < bound) & (pos >= bound - WINDOW)
            rows = pl.ds(pl.multiple_of(origin * block_rows, block_rows), block_rows)

            for h, out in enumerate((ck_ref, cv_ref)):

                def put(g, value):
                    cols = pl.ds(pl.multiple_of(g * HD, HD), HD)
                    out[rows, cols] = jnp.where(live, value.astype(jnp.float32), 0.0).astype(
                        jnp.bfloat16
                    )

                @pl.when(zo > z)
                def _():
                    for g in (0, 1):
                        put(g, down_in[origin, h, g])

                @pl.when(zo <= z)
                def _():
                    put(1 - y, pair_in[zo, yo, h])

                @pl.when((zo <= z) & jnp.logical_not(far))
                def _():
                    put(y, select(kv, (origin, h), mine_blocks))

                @pl.when(far)
                def _():
                    put(y, line_in[zo, yo, h])

        return carry

    lax.fori_loop(0, nz, cache, 0)
    rest = ck_ref.shape[0] - n * block_rows
    if rest:
        for out in (ck_ref, cv_ref):
            out[n * block_rows :, :] = jnp.zeros((rest, 2 * HD), jnp.bfloat16)
    settle(from_sib2, sib2_recv)
    for r in range(chunks):
        x_copy(r).wait_recv()
        rows = slice(r * ROWS, (r + 1) * ROWS)
        branch = total[rows, :] + from_sib2[r].astype(jnp.float32) + from_x[r].astype(jnp.float32)
        total[rows, :] = branch
        squared = branch * branch
        folded = squared[:, :LANES]
        for i in range(1, width // LANES):
            folded = folded + squared[:, i * LANES : (i + 1) * LANES]
        folds[rows, :] = folded
        if (r + 1) * ROWS % LANES == 0:
            rows = slice((r + 1) * ROWS - LANES, (r + 1) * ROWS)
            line = jnp.sum(folds[rows, :].T, axis=0, keepdims=True)
            sq_out[:, rows] = jnp.broadcast_to(line, (8, LANES))

    def sq_copy(i, to, slot):
        return pltpu.make_async_remote_copy(
            src_ref=sq_out, dst_ref=sq_in.at[slot], send_sem=sq_send.at[0],
            recv_sem=sq_recv.at[0], device_id={"tp": to}, device_id_type=MESH,
        )

    peers = (sib, across, diagonal)
    for i, peer in enumerate(peers):
        sq_copy(i, peer, t).start()
    squares = sq_out[...]
    settle(sq_in.at[:3], sq_recv)
    for i, peer in enumerate(peers):
        squares = squares + sq_in[peer]
    loads[7].wait()
    loads[8].wait()
    factor = lax.rsqrt(squares / D + norm_eps)
    for r in range(shard // LANES):
        rows = slice(r * LANES, (r + 1) * LANES)
        spread = jnp.broadcast_to(factor[:1, rows], (LANES, LANES)).T
        for i in range(width // LANES):
            cols = slice(i * LANES, (i + 1) * LANES)
            normed = total[rows, cols] * spread * scale_ref[cols].reshape(1, LANES)
            hid_ref[rows, cols] = (res_ref[rows, cols].astype(jnp.float32) + normed).astype(
                jnp.bfloat16
            )

    settle(sq_in.at[:3], sq_send)
    for kind, sent_rows in enumerate((to_sib, to_x, to_sib2)):
        pltpu.make_async_copy(sent_rows, sent_rows, rs_send.at[kind]).wait()
    settle(other, y_send)
    settle(qpart, yq_send)
    for slab in range(nz):

        @pl.when((z == slab) & sends_kv)
        def _():
            settle(kv.at[: 2 * slab + 2], z_send)

        @pl.when((z == slab) & takes_kv)
        def _():
            settle(pair_out.at[: slab + 1], pair_send)

        if slab:

            @pl.when(z == slab)
            def _():
                settle(down_out.at[: 2 * slab], down_send)

    @pl.when(lends)
    def _():
        settle(qall.at[:2], q_send)
        settle(kv.at[2 * top :], z_send)
        settle(pair_out.at[top:], pair_send)

    @pl.when(jnp.logical_not(lends))
    def _():
        settle(att_out, att_send)

    @pl.when(hosts)
    def _():
        settle(lent_out, lent_send)
        settle(line_out.at[:top], line_send)
        settle(skew_out.at[:top], skew_send)


def put_out(*refs):
    count = (len(refs) - 1) // 2
    copies = [
        pltpu.make_async_copy(refs[i], refs[count + i], refs[-1].at[i]) for i in range(count)
    ]
    for copy in copies:
        copy.start()
    for copy in copies:
        copy.wait()


def fused(n, queries, key_rows, value_rows, residual, out_weight, post_scale, lengths, owners):
    shard, q_width = queries.shape[1:]
    kv_width = key_rows.shape[2]
    width = residual.shape[2]
    chunks = shard // ROWS
    cache_rows = WINDOW // n
    smem = pl.BlockSpec(memory_space=pltpu.SMEM)
    apart = pl.BlockSpec(memory_space=pl.ANY)
    held = pl.BlockSpec(memory_space=pltpu.VMEM)
    one = pltpu.SemaphoreType.DMA((1,))
    group_cols = q_width * HD // kv_width
    slab = pltpu.VMEM((n // 2, 2, 2, shard // n, HD), jnp.bfloat16)
    half = pltpu.VMEM((chunks, ROWS, width), jnp.bfloat16)
    hidden, ck, cv = pl.pallas_call(
        functools.partial(layer_kernel, n),
        out_shape=(
            pltpu.VMEM((shard, width), jnp.bfloat16),
            pltpu.VMEM((cache_rows, kv_width), jnp.bfloat16),
            pltpu.VMEM((cache_rows, kv_width), jnp.bfloat16),
        ),
        in_specs=[apart] * 5 + [smem] + [apart] * 2,
        out_specs=(held,) * 3,
        scratch_shapes=[
            pltpu.VMEM((4, shard, group_cols), jnp.bfloat16),
            pltpu.VMEM((shard, group_cols), jnp.bfloat16),
            pltpu.VMEM((shard, width), jnp.bfloat16),
            pltpu.VMEM((width,), jnp.float32),
            pltpu.SMEM((1, n), jnp.int32),
            pltpu.VMEM((n, 2, shard, HD), jnp.bfloat16),
            pltpu.VMEM((2, shard, HD), jnp.bfloat16),
            pltpu.VMEM((n, 2, 2, shard // n, HD), jnp.bfloat16),
            pltpu.VMEM((n, 2, 2, shard // n, HD), jnp.bfloat16),
            slab, slab, slab, slab, slab,
            pltpu.VMEM((4, 2, group_cols, width), jnp.bfloat16),
            pltpu.VMEM((group_cols // HD, 4, shard, HD), jnp.float32),
            pltpu.VMEM((group_cols // HD, 4, shard, LANES), jnp.float32),
            pltpu.VMEM((2, chunks, ROWS, group_cols), jnp.bfloat16),
            pltpu.VMEM((chunks, ROWS, group_cols), jnp.bfloat16),
            pltpu.VMEM((2, chunks, ROWS, group_cols), jnp.bfloat16),
            half, half, half, half, half, half,
            pltpu.VMEM((2, shard, width), jnp.float32),
            pltpu.VMEM((shard, width), jnp.float32),
            pltpu.VMEM((shard, LANES), jnp.float32),
            pltpu.VMEM((8, shard), jnp.float32),
            pltpu.VMEM((4, 8, shard), jnp.float32),
            pltpu.SemaphoreType.DMA((9,)),
            one,
            one,
            one,
            pltpu.SemaphoreType.DMA((3,)),
            one,
            pltpu.SemaphoreType.DMA((n - 2, 2)),
            one,
            one,
            one,
            one,
            one,
            one,
            one,
            one,
            one,
            one,
            one,
            one,
            pltpu.SemaphoreType.DMA((chunks,)),
            pltpu.SemaphoreType.DMA((3,)),
            pltpu.SemaphoreType.DMA((2, chunks)),
            one,
            one,
            one,
        ],
        compiler_params=pltpu.CompilerParams(
            collective_id=0, has_side_effects=True, vmem_limit_bytes=62 * 1024 * 1024
        ),
    )(
        queries[0], key_rows[0], value_rows[0], residual[0], post_scale, lengths, owners,
        out_weight,
    )
    made = (hidden, ck, cv)
    hidden, ck, cv = pl.pallas_call(
        put_out,
        out_shape=tuple(jax.ShapeDtypeStruct(a.shape, a.dtype) for a in made),
        in_specs=[apart] * len(made),
        out_specs=(apart,) * len(made),
        scratch_shapes=[pltpu.SemaphoreType.DMA((len(made),))],
    )(*(pltpu.with_memory_space_constraint(a, pltpu.VMEM) for a in made))
    return hidden[None], ck[None], cv[None]


def solution(mesh):
    placed = (
        P(None, "seq", "tp"),
        P(None, "seq", "tp"),
        P(None, "seq", "tp"),
        P(None, "seq", "tp"),
        P("tp", None),
        P("tp"),
        P(),
        P(),
    )
    return jax.shard_map(
        local,
        mesh=mesh,
        in_specs=placed,
        out_specs=(P(None, "seq", "tp"), P(None, "seq", "tp"), P(None, "seq", "tp")),
        check_vma=False,
    )
```

```python
import functools

import jax
import jax.numpy as jnp
from jax import lax
from jax.experimental import pallas as pl
from jax.experimental.pallas import tpu as pltpu
from jax.sharding import PartitionSpec as P

D = 3584
HD = 256
WINDOW = 4096
MESH = pl.DeviceIdType.MESH
LOG2E = 1.4426950408889634
ROWS = 32
LANES = 128


soft_cap = 50.0
norm_eps = 1e-06


def shifted(x, axis, by):
    peers = lax.axis_size(axis)
    pairs = [(i, i + by) for i in range(peers) if 0 <= i + by < peers]
    return lax.ppermute(x, axis, pairs)


def attend_block(grouped, block_keys, block_values, query_pos, key_pos, state_pair):
    numerator, denominator = state_pair
    seq_count, query_count, kv_local, group_size, head_size = grouped.shape
    keyed_rows = block_keys.reshape(seq_count, block_keys.shape[1], kv_local, head_size)
    valued_rows = block_values.reshape(seq_count, block_values.shape[1], kv_local, head_size)
    scores = jnp.einsum(
        "sqhgd,skhd->shgqk", grouped, keyed_rows, preferred_element_type=jnp.float32
    ) * head_size ** (-0.5)
    capped = soft_cap * jnp.tanh(scores / soft_cap)
    spread = query_pos[:, None] - key_pos[None, :]
    live_mask = (spread >= 0) & (spread < WINDOW) & (key_pos[None, :] >= 0)
    weights = jnp.where(live_mask, jnp.exp(capped), jnp.zeros_like(capped))
    denominator = denominator + jnp.sum(weights, axis=-1)
    numerator = numerator + jnp.einsum(
        "shgqk,skhd->sqhgd",
        weights.astype(jnp.bfloat16),
        valued_rows,
        preferred_element_type=jnp.float32,
    )
    return (numerator, denominator)


def reorder_blocks(blocked, ordering):
    return blocked[ordering]


def local(queries, key_rows, value_rows, residual, out_weight, post_scale, lengths, owners):
    seq_count, shard_len, query_width = queries.shape
    seq_size = lax.axis_size("seq")
    if (
        seq_count == 1 and lax.axis_size("tp") == 4 and seq_size % 2 == 0 and seq_size >= 8
        and seq_size * shard_len <= WINDOW and key_rows.shape[2] == 2 * HD
        and shard_len % LANES == 0
    ):
        return fused(
            seq_size, queries, key_rows, value_rows, residual, out_weight, post_scale, lengths,
            owners,
        )
    kv_width = key_rows.shape[2]
    kv_local = kv_width // HD
    group_size = query_width // kv_width
    grouped = queries.reshape(seq_count, shard_len, kv_local, group_size, HD)
    position = lax.axis_index("seq")
    seq_devices = lax.axis_size("seq")
    offsets = jnp.arange(shard_len, dtype=jnp.int32)
    query_pos = position * shard_len + offsets
    numerator = jnp.zeros((seq_count, shard_len, kv_local, group_size, HD), jnp.float32)
    denominator = jnp.zeros((seq_count, kv_local, group_size, shard_len), jnp.float32)
    state_pair = attend_block(
        grouped, key_rows, value_rows, query_pos, query_pos, (numerator, denominator)
    )
    hop_count = min(WINDOW // shard_len, seq_devices - 1)
    arrived = []
    current = (key_rows, value_rows)
    for hop_index in range(1, hop_count + 1):
        current = shifted((current[0], current[1]), "seq", 1)
        arrived.append((hop_index, current))
        if len(arrived) == 2 or hop_index == hop_count:
            ordered = arrived[::-1]
            block_keys = jnp.concatenate([member[1][0] for member in ordered], axis=1)
            block_values = jnp.concatenate([member[1][1] for member in ordered], axis=1)
            block_pos = jnp.concatenate(
                [(position - member[0]) * shard_len + offsets for member in ordered]
            )
            state_pair = attend_block(
                grouped, block_keys, block_values, query_pos, block_pos, state_pair
            )
            arrived = []
    numerator, denominator = state_pair
    attended = (numerator / jnp.transpose(denominator, (0, 3, 1, 2))[..., None]).astype(
        jnp.bfloat16
    )
    partial_value = jnp.dot(
        attended.reshape(seq_count * shard_len, query_width),
        out_weight,
        preferred_element_type=jnp.float32,
    )
    partial_value = partial_value.reshape(seq_count, shard_len, out_weight.shape[1])
    branch = lax.psum_scatter(partial_value, "tp", scatter_dimension=2, tiled=True)
    squares = lax.psum(jnp.sum(branch * branch, axis=-1), "tp")
    normed = branch * lax.rsqrt(squares / D + norm_eps)[..., None] * post_scale
    hidden_out = (residual.astype(jnp.float32) + normed).astype(jnp.bfloat16)
    block_rows = shard_len // seq_devices
    slot_span = WINDOW // shard_len
    live_rows = (query_pos[None, :] >= lengths[:, None] - WINDOW) & (
        query_pos[None, :] < lengths[:, None]
    )
    kept_keys = jnp.where(live_rows[..., None], key_rows, jnp.zeros_like(key_rows))
    kept_values = jnp.where(live_rows[..., None], value_rows, jnp.zeros_like(value_rows))
    devices = jnp.arange(seq_devices, dtype=jnp.int32)
    matches = owners[:, :, None] == devices[None, None, :]
    inverse = jnp.sum(
        jnp.where(matches, devices[None, :, None], jnp.zeros_like(devices)[None, :, None]), axis=1
    )
    outgoing_keys = jax.vmap(reorder_blocks)(
        kept_keys.reshape(seq_count, seq_devices, block_rows, kv_width), inverse
    )
    outgoing_values = jax.vmap(reorder_blocks)(
        kept_values.reshape(seq_count, seq_devices, block_rows, kv_width), inverse
    )
    incoming = (
        lax.all_to_all(outgoing_keys, "seq", split_axis=1, concat_axis=1, tiled=True),
        lax.all_to_all(outgoing_values, "seq", split_axis=1, concat_axis=1, tiled=True),
    )
    selector = (
        devices[None, :] % slot_span == jnp.arange(slot_span, dtype=jnp.int32)[:, None]
    ).astype(jnp.bfloat16)
    cache_keys = (
        jnp.einsum("md,sdbf->smbf", selector, incoming[0], preferred_element_type=jnp.float32)
        .astype(jnp.bfloat16)
        .reshape(seq_count, slot_span * block_rows, kv_width)
    )
    cache_values = (
        jnp.einsum("md,sdbf->smbf", selector, incoming[1], preferred_element_type=jnp.float32)
        .astype(jnp.bfloat16)
        .reshape(seq_count, slot_span * block_rows, kv_width)
    )
    return (hidden_out, cache_keys, cache_values)


def layer_kernel(
    n, q_hbm, k_hbm, v_hbm, res_hbm, scale_hbm, len_ref, own_hbm, w_ref,
    hid_ref, ck_ref, cv_ref,
    qall, qpart, res_ref, scale_ref, own_ref, kv, other,
    down_out, down_in, pair_out, pair_in, line_out, line_in, skew_out,
    wbuf, acc, den, rounded, att, att_out, lent_out,
    to_sib, to_x, to_sib2, from_sib, from_x, from_sib2, early, total, folds, sq_out, sq_in,
    in_sem, w_sem, y_send, yq_send, y_recv, z_send, z_recv, lend_recv, q_send, q_recv, lent_send,
    down_send, down_recv, pair_send, pair_recv, line_send, line_recv, skew_send, att_send, att_recv,
    rs_send, rs_recv, sib2_recv, sq_send, sq_recv, turn,
):
    nz = n // 2
    top = nz - 1
    me = lax.axis_index("seq")
    t = lax.axis_index("tp")
    z, y = me // 2, me % 2
    x, c = t // 2, t % 2
    sib = x * 2 + (1 - c)
    across = (1 - x) * 2 + c
    diagonal = (1 - x) * 2 + (1 - c)
    partner = z * 2 + (1 - y)
    shard = kv.shape[2]
    width = res_ref.shape[1]
    group_cols = qpart.shape[1]
    group = group_cols // HD
    block_rows = shard // n
    chunks = shard // ROWS
    merge = LANES // ROWS
    lends = (c == 1) & (z == top)
    hosts = (c == 1) & (z == top - 1)
    takes_kv = (z < top) | (c == 0)
    sends_kv = (z < top - 1) | ((z < top) & (c == 0))

    frees = (c == 0) & (z == top - 2)
    defers = (c == 1) & (z == top - 2)

    def half(ref, which, cols):
        return ref.at[:, pl.ds(pl.multiple_of(which * cols, cols), cols)]

    loads = [
        pltpu.make_async_copy(src, dst, in_sem.at[i])
        for i, (src, dst) in enumerate(
            (
                (half(k_hbm, 1 - y, HD), other.at[0]), (half(v_hbm, 1 - y, HD), other.at[1]),
                (half(k_hbm, y, HD), kv.at[me, 0]), (half(v_hbm, y, HD), kv.at[me, 1]),
                (half(q_hbm, 1 - y, group_cols), qpart), (half(q_hbm, y, group_cols), qall.at[y]),
                (own_hbm, own_ref), (res_hbm, res_ref), (scale_hbm, scale_ref),
            )
        )
    ]
    for load in loads[:7]:
        load.start()

    barrier = pltpu.get_barrier_semaphore()
    for peer in (sib, across, diagonal):
        pl.semaphore_signal(barrier, inc=1, device_id={"tp": peer}, device_id_type=MESH)
    for hop in range(1, n):
        pl.semaphore_signal(
            barrier, inc=1, device_id={"seq": lax.rem(me + hop, n)}, device_id_type=MESH
        )

    def clear(s, carry):
        acc[s] = jnp.zeros(acc.shape[1:], jnp.float32)
        den[s] = jnp.zeros(den.shape[1:], jnp.float32)
        return carry

    lax.fori_loop(0, acc.shape[0], clear, 0)
    pl.semaphore_wait(barrier, n + 2)

    def remote(src, dst, send, recv, to):
        return pltpu.make_async_remote_copy(
            src_ref=src, dst_ref=dst, send_sem=send, recv_sem=recv, device_id=to,
            device_id_type=MESH,
        )

    def settle(ref, sem):
        pltpu.make_async_copy(ref, ref, sem.at[0]).wait()

    def y_copy(h, origin):
        return remote(
            other.at[h], kv.at[origin, h], y_send.at[0], y_recv.at[h], {"seq": partner}
        )

    def yq_copy(slot):
        return remote(qpart, qall.at[slot], yq_send.at[0], y_recv.at[2], {"seq": partner})

    def z_copy(origin, h):
        return remote(
            kv.at[origin, h], kv.at[origin, h], z_send.at[0], z_recv.at[origin, h],
            {"seq": me + 2},
        )

    def lend_copy(yq):
        return remote(
            qall.at[yq], qall.at[2 + yq], q_send.at[0], q_recv.at[0], {"seq": me - 2}
        )

    def lend_kv(origin, h):
        return remote(
            kv.at[origin, h], kv.at[origin, h], z_send.at[0], lend_recv.at[0],
            {"seq": me - 2},
        )

    def w_copy(f, g):
        return pltpu.make_async_copy(
            w_ref.at[pl.ds(g * group_cols, group_cols), pl.ds(f * width, width)],
            wbuf.at[f, g], w_sem.at[0],
        )

    for h in (0, 1):
        loads[2 + h].wait()
        pl.when(sends_kv)(z_copy(me, h).start)
    for load in (loads[0], loads[1], loads[4], loads[5]):
        load.wait()

    @pl.when(z == top)
    def _():
        yq_copy(y).start()
        for h in (0, 1):
            y_copy(h, me).start()

    @pl.when(z < top)
    def _():
        for h in (0, 1):
            y_copy(h, me).start()
        yq_copy(y).start()

    @pl.when(lends)
    def _():
        lend_copy(y).start()
        for h in (0, 1):
            lend_kv(me, h).start()

    loads[6].wait()
    for f in range(4):
        for g in (0, 1):
            w_copy(f, g).start()
    for load in loads[7:]:
        load.start()

    def owned(device):
        block = own_ref[0, 0] * 0
        for b in range(n):
            block = block + jnp.where(own_ref[0, b] == device, b, 0)
        return jnp.full((block_rows, HD), block, jnp.int32)

    def select(ref, lead, chosen):
        got = jnp.zeros(chosen.shape, jnp.float32)
        for b in range(n):
            rows = ref[(*lead, slice(b * block_rows, (b + 1) * block_rows))]
            got = jnp.where(chosen == b, rows.astype(jnp.float32), got)
        return got.astype(jnp.bfloat16)

    def down_copy(to, slot):
        return remote(
            down_out.at[to], down_in.at[slot], down_send.at[0], down_recv.at[0], {"seq": to}
        )

    def stage(to, carry):
        chosen = owned(to)
        for h in (0, 1):
            down_out[to, h, y] = select(kv, (me, h), chosen)
            down_out[to, h, 1 - y] = select(other, (h,), chosen)
        return carry

    def post(to, carry):
        down_copy(to, me).start()
        return carry

    lax.fori_loop(0, 2 * z, stage, 0)

    def pair_copy(zo):
        return remote(
            pair_out.at[zo], pair_in.at[zo], pair_send.at[0], pair_recv.at[0], {"seq": partner}
        )

    def line_copy(zo):
        return remote(
            line_out.at[zo], line_in.at[zo], line_send.at[0], line_recv.at[0], {"seq": me + 2}
        )

    def skew_copy(zo):
        return remote(
            skew_out.at[zo], pair_in.at[zo], skew_send.at[0], pair_recv.at[0],
            {"seq": partner + 2},
        )

    def gather(zo, device, out):
        chosen = owned(device)
        for yo in (0, 1):
            for h in (0, 1):
                out[zo, yo, h] = select(kv, (2 * zo + yo, h), chosen)

    def pass_cache(zo):
        @pl.when((zo == z) | takes_kv)
        def _():
            gather(zo, partner, pair_out)
            pair_copy(zo).start()

    def lift_cache(zo):
        gather(zo, me + 2, line_out)
        line_copy(zo).start()
        gather(zo, partner + 2, skew_out)
        skew_copy(zo).start()

    @pl.when(lends)
    def _():
        yq_copy(1 - y).wait_recv()
        lend_copy(1 - y).start()

    for h in (0, 1):
        y_copy(h, partner).wait_recv()
        pl.when(sends_kv)(z_copy(partner, h).start)
        pl.when(lends)(lend_kv(partner, h).start)
    lax.fori_loop(0, 2 * z, post, 0)

    pl.when(hosts)(functools.partial(lift_cache, z))

    def take(origin, h):
        z_copy(origin, h).wait_recv()
        held_back = defers & (origin == 1 - y)
        pl.when(sends_kv & jnp.logical_not(held_back))(z_copy(origin, h).start)

    @pl.when((z > 0) & takes_kv)
    def _():
        for origin in (me - 2, partner - 2):
            for h in (0, 1):
                take(origin, h)

    @pl.when(hosts & (z > 1))
    def _():
        lift_cache(z - 1)

    @pl.when(jnp.logical_not(lends))
    def _():
        yq_copy(1 - y).wait_recv()

    def attend(base, origin, above):
        pair = pl.ds(base, 2)
        for hh in range(group):
            stacked = qall[pair, :, hh * HD : (hh + 1) * HD].reshape(2 * shard, HD)
            scores = lax.dot_general(
                stacked, kv[origin, 0], (((1,), (1,)), ((), ())),
                preferred_element_type=jnp.float32,
            )
            w = jnp.exp2(jnp.tanh(scores * (HD ** (-0.5) / soft_cap)) * (soft_cap * LOG2E))
            if above is not None:
                keep = lax.broadcasted_iota(jnp.int32, w.shape, 0) >= above + (
                    lax.broadcasted_iota(jnp.int32, w.shape, 1)
                )
                w = jnp.where(keep, w, 0.0)
            folded = w[:, :LANES]
            for i in range(1, w.shape[1] // LANES):
                folded = folded + w[:, i * LANES : (i + 1) * LANES]
            den[hh, pair] += folded.reshape(2, shard, LANES)
            acc[hh, pair] += jnp.dot(
                w.astype(jnp.bfloat16), kv[origin, 1], preferred_element_type=jnp.float32
            ).reshape(2, shard, HD)

    def weigh(i, origin):
        pair = pl.ds(2 * i, 2)
        for hh in range(group):
            stacked = qall[pair, :, hh * HD : (hh + 1) * HD].reshape(2 * shard, HD)
            scores = lax.dot_general(
                stacked, kv[origin, 0], (((1,), (1,)), ((), ())),
                preferred_element_type=jnp.float32,
            )
            w = jnp.exp2(jnp.tanh(scores * (HD ** (-0.5) / soft_cap)) * (soft_cap * LOG2E))
            folded = w[:, :LANES]
            for j in range(1, w.shape[1] // LANES):
                folded = folded + w[:, j * LANES : (j + 1) * LANES]
            den[hh, pair] += folded.reshape(2, shard, LANES)
            rounded[i, hh] = w.astype(jnp.bfloat16)

    def mix(i, origin):
        pair = pl.ds(2 * i, 2)
        for hh in range(group):
            acc[hh, pair] += jnp.dot(
                rounded[i, hh], kv[origin, 1], preferred_element_type=jnp.float32
            ).reshape(2, shard, HD)

    def invert():
        def one(i, carry):
            pair = pl.ds(2 * i, 2)
            for hh in range(group):
                whole = den[hh, pair].reshape(2 * shard, LANES)
                inverse = 1.0 / jnp.sum(whole, axis=-1, keepdims=True)
                den[hh, pair] = jnp.broadcast_to(inverse, whole.shape).reshape(2, shard, LANES)
            return carry

        lax.fori_loop(0, jnp.where(hosts, 2, 1), one, 0)

    def own_slab(base, slab):
        def diagonal_block(i, carry):
            attend(base, 2 * slab + i, i * shard)
            return carry

        lax.fori_loop(0, 2, diagonal_block, 0)

    pl.when(jnp.logical_not(lends))(functools.partial(own_slab, 0, z))
    @pl.when(hosts)
    def _():
        settle(qall.at[2:], q_recv)

        def one(i, carry):
            attend(2, 2 * z + i, None)
            return carry

        lax.fori_loop(0, 2, one, 0)

    pairs = jnp.where(hosts, 2, 1)

    def phase(d, carry):
        @pl.when(z - d + 1 >= 1)
        def _():
            pass_cache(z - d + 1)

        @pl.when(hosts & (d > 2) & (z - d + 1 >= 1))
        def _():
            lift_cache(z - d + 1)

        @pl.when(hosts & (d == jnp.minimum(2, z)))
        def _():
            settle(kv.at[2 * top :], lend_recv)
            own_slab(2, top)

        def side(j, carry):
            @pl.when((z - d >= 0) & takes_kv)
            def _():
                origin = 2 * (z - d) + jnp.where(j == 0, y, 1 - y)
                for h, work in enumerate((weigh, mix)):
                    pl.when(d > 1)(functools.partial(take, origin, h))

                    def one(i, carry):
                        work(i, origin)
                        return carry

                    lax.fori_loop(0, pairs, one, 0)
                    if h == 0:
                        pl.when((d == z) & (j == 1))(invert)

            return carry

        lax.fori_loop(0, 2, side, 0)
        return carry

    lax.fori_loop(1, nz, phase, 0)

    pl.when(z == 0)(invert)

    @pl.when(frees)
    def _():
        settle(kv.at[: 2 * top - 2], z_send)
        pl.semaphore_signal(turn, inc=1, device_id={"tp": sib}, device_id_type=MESH)

    @pl.when(defers)
    def _():
        pl.semaphore_wait(turn, 1)
        for h in (0, 1):
            z_copy(1 - y, h).start()

    def rows_of(r):
        return pl.ds(pl.multiple_of(r * ROWS, ROWS), ROWS)

    def att_copy(r, g):
        return remote(
            att_out.at[r], att.at[g, r], att_send.at[0], att_recv.at[r], {"seq": partner}
        )

    def lent_copy(yq, r, g):
        return remote(
            lent_out.at[yq, r], att.at[g, r], lent_send.at[0], att_recv.at[r],
            {"seq": 2 * top + yq},
        )

    def finish(s, r, out, lead):
        for hh in range(group):
            for i in range(HD // LANES):
                cols = slice(i * LANES, (i + 1) * LANES)
                out[(*lead, slice(None), slice(hh * HD + i * LANES, hh * HD + (i + 1) * LANES))] = (
                    acc[hh, s, rows_of(r), cols] * den[hh, s, rows_of(r), :]
                ).astype(jnp.bfloat16)

    def away(r, carry):
        finish(1 - y, r, att_out, (r,))
        att_copy(r, y).start()
        return carry

    def home(r, carry):
        finish(y, r, att, (y, r))
        return carry

    def give(r, carry):
        for yq in (1 - y, y):
            finish(2 + yq, r, lent_out, (yq, r))
            lent_copy(yq, r, y).start()
        return carry

    def both_slabs(r, carry):
        give(r, carry)
        return away(r, carry)

    @pl.when(hosts)
    def _():
        lax.fori_loop(0, chunks, both_slabs, 0)

    @pl.when(jnp.logical_not(lends | hosts))
    def _():
        lax.fori_loop(0, chunks, away, 0)

    @pl.when(jnp.logical_not(lends))
    def _():
        lax.fori_loop(0, chunks, home, 0)

    def rs_copy(kind, r, src, dst, recv, to):
        return remote(src.at[r], dst.at[r], rs_send.at[kind], recv, {"tp": to})

    def sib_copy(r):
        return rs_copy(0, r, to_sib, from_sib, rs_recv.at[0, r], sib)

    def x_copy(r):
        return rs_copy(1, r, to_x, from_x, rs_recv.at[1, r], across)

    def sib2_copy(r):
        return rs_copy(2, r, to_sib2, from_sib2, sib2_recv.at[0], sib)

    def product(rows, f, g):
        return jnp.dot(rows, wbuf[f, g], preferred_element_type=jnp.float32)

    def part(f, r):
        some = pl.ds(merge * r, merge)
        rows = [att[g, some].reshape(LANES, group_cols) for g in (0, 1)]
        return product(rows[0], f, 0) + product(rows[1], f, 1)

    settle(wbuf, w_sem)

    sent = (diagonal, across)

    @pl.when(jnp.logical_not(lends))
    def _():
        for i, f in enumerate(sent):
            early[i] = product(att[y].reshape(shard, group_cols), f, y)

    def send_sib(r):
        pl.when(jnp.logical_not(lends))(att_copy(r, 1 - y).wait_recv)

        @pl.when(lends)
        def _():
            both_heads = att.at[:, r]
            pltpu.make_async_copy(both_heads, both_heads, att_recv.at[r]).wait()
            early[0, rows_of(r), :] = product(att[y, r], diagonal, y)

        to_sib[r] = (early[0, rows_of(r), :] + product(att[1 - y, r], diagonal, 1 - y)).astype(
            jnp.bfloat16
        )
        sib_copy(r).start()

    def send_x(r):
        @pl.when(lends)
        def _():
            early[1, rows_of(r), :] = product(att[y, r], across, y)

        mine = early[1, rows_of(r), :] + product(att[1 - y, r], across, 1 - y)
        sib_copy(r).wait_recv()
        to_x[r] = (mine + from_sib[r].astype(jnp.float32)).astype(jnp.bfloat16)
        x_copy(r).start()

    def both(r, carry):
        pl.when(r < chunks)(functools.partial(send_sib, r))
        pl.when(r > 0)(functools.partial(send_x, r - 1))
        return carry

    def third(r, carry):
        some = pl.ds(merge * r, merge)
        to_sib2[some] = part(sib, r).astype(jnp.bfloat16).reshape(merge, ROWS, width)
        for i in range(merge):
            sib2_copy(merge * r + i).start()
        return carry

    def fourth(r, carry):
        rows = pl.ds(pl.multiple_of(r * LANES, LANES), LANES)
        total[rows, :] = part(t, r)
        return carry

    lax.fori_loop(0, chunks + 1, both, 0)

    pass_cache(0)
    pl.when(hosts)(functools.partial(lift_cache, 0))

    for step in (third, fourth):
        lax.fori_loop(0, chunks // merge, step, 0)

    mine_blocks = owned(me)
    local_row = lax.broadcasted_iota(jnp.int32, mine_blocks.shape, 0)
    bound = jnp.full(mine_blocks.shape, len_ref[0], jnp.int32)

    for slab in range(nz):

        @pl.when(z == slab)
        def _():
            settle(pair_in.at[: slab + 1], pair_recv)
            if slab < top:
                settle(down_in.at[2 * slab + 2 :], down_recv)

    @pl.when(lends)
    def _():
        settle(line_in.at[:top], line_recv)

    def cache(zo, carry):
        far = lends & (zo < top)

        for yo in (0, 1):
            origin = 2 * zo + yo
            pos = local_row + mine_blocks * block_rows + origin * shard
            live = (pos < bound) & (pos >= bound - WINDOW)
            rows = pl.ds(pl.multiple_of(origin * block_rows, block_rows), block_rows)

            for h, out in enumerate((ck_ref, cv_ref)):

                def put(g, value):
                    cols = pl.ds(pl.multiple_of(g * HD, HD), HD)
                    out[rows, cols] = jnp.where(live, value.astype(jnp.float32), 0.0).astype(
                        jnp.bfloat16
                    )

                @pl.when(zo > z)
                def _():
                    for g in (0, 1):
                        put(g, down_in[origin, h, g])

                @pl.when(zo <= z)
                def _():
                    put(1 - y, pair_in[zo, yo, h])

                @pl.when((zo <= z) & jnp.logical_not(far))
                def _():
                    put(y, select(kv, (origin, h), mine_blocks))

                @pl.when(far)
                def _():
                    put(y, line_in[zo, yo, h])

        return carry

    lax.fori_loop(0, nz, cache, 0)
    rest = ck_ref.shape[0] - n * block_rows
    if rest:
        for out in (ck_ref, cv_ref):
            out[n * block_rows :, :] = jnp.zeros((rest, 2 * HD), jnp.bfloat16)
    settle(from_sib2, sib2_recv)
    for r in range(chunks):
        x_copy(r).wait_recv()
        rows = slice(r * ROWS, (r + 1) * ROWS)
        branch = total[rows, :] + from_sib2[r].astype(jnp.float32) + from_x[r].astype(jnp.float32)
        total[rows, :] = branch
        squared = branch * branch
        folded = squared[:, :LANES]
        for i in range(1, width // LANES):
            folded = folded + squared[:, i * LANES : (i + 1) * LANES]
        folds[rows, :] = folded
        if (r + 1) * ROWS % LANES == 0:
            rows = slice((r + 1) * ROWS - LANES, (r + 1) * ROWS)
            line = jnp.sum(folds[rows, :].T, axis=0, keepdims=True)
            sq_out[:, rows] = jnp.broadcast_to(line, (8, LANES))

    def sq_copy(i, to, slot):
        return pltpu.make_async_remote_copy(
            src_ref=sq_out, dst_ref=sq_in.at[slot], send_sem=sq_send.at[0],
            recv_sem=sq_recv.at[0], device_id={"tp": to}, device_id_type=MESH,
        )

    peers = (sib, across, diagonal)
    for i, peer in enumerate(peers):
        sq_copy(i, peer, t).start()
    squares = sq_out[...]
    settle(sq_in.at[:3], sq_recv)
    for i, peer in enumerate(peers):
        squares = squares + sq_in[peer]
    loads[7].wait()
    loads[8].wait()
    factor = lax.rsqrt(squares / D + norm_eps)
    for r in range(shard // LANES):
        rows = slice(r * LANES, (r + 1) * LANES)
        spread = jnp.broadcast_to(factor[:1, rows], (LANES, LANES)).T
        for i in range(width // LANES):
            cols = slice(i * LANES, (i + 1) * LANES)
            normed = total[rows, cols] * spread * scale_ref[cols].reshape(1, LANES)
            hid_ref[rows, cols] = (res_ref[rows, cols].astype(jnp.float32) + normed).astype(
                jnp.bfloat16
            )

    settle(sq_in.at[:3], sq_send)
    for kind, sent_rows in enumerate((to_sib, to_x, to_sib2)):
        pltpu.make_async_copy(sent_rows, sent_rows, rs_send.at[kind]).wait()
    settle(other, y_send)
    settle(qpart, yq_send)
    for slab in range(nz):

        @pl.when((z == slab) & sends_kv & jnp.logical_not(frees))
        def _():
            settle(kv.at[: 2 * slab + 2], z_send)

        @pl.when((z == slab) & takes_kv)
        def _():
            settle(pair_out.at[: slab + 1], pair_send)

        if slab:

            @pl.when(z == slab)
            def _():
                settle(down_out.at[: 2 * slab], down_send)

    @pl.when(lends)
    def _():
        settle(qall.at[:2], q_send)
        settle(kv.at[2 * top :], z_send)
        settle(pair_out.at[top:], pair_send)

    @pl.when(jnp.logical_not(lends))
    def _():
        settle(att_out, att_send)

    @pl.when(hosts)
    def _():
        settle(lent_out, lent_send)
        settle(line_out.at[:top], line_send)
        settle(skew_out.at[:top], skew_send)


def put_out(*refs):
    count = (len(refs) - 1) // 2
    copies = [
        pltpu.make_async_copy(refs[i], refs[count + i], refs[-1].at[i]) for i in range(count)
    ]
    for copy in copies:
        copy.start()
    for copy in copies:
        copy.wait()


def fused(n, queries, key_rows, value_rows, residual, out_weight, post_scale, lengths, owners):
    shard, q_width = queries.shape[1:]
    kv_width = key_rows.shape[2]
    width = residual.shape[2]
    chunks = shard // ROWS
    cache_rows = WINDOW // n
    smem = pl.BlockSpec(memory_space=pltpu.SMEM)
    apart = pl.BlockSpec(memory_space=pl.ANY)
    held = pl.BlockSpec(memory_space=pltpu.VMEM)
    one = pltpu.SemaphoreType.DMA((1,))
    group_cols = q_width * HD // kv_width
    slab = pltpu.VMEM((n // 2, 2, 2, shard // n, HD), jnp.bfloat16)
    half = pltpu.VMEM((chunks, ROWS, width), jnp.bfloat16)
    hidden, ck, cv = pl.pallas_call(
        functools.partial(layer_kernel, n),
        out_shape=(
            pltpu.VMEM((shard, width), jnp.bfloat16),
            pltpu.VMEM((cache_rows, kv_width), jnp.bfloat16),
            pltpu.VMEM((cache_rows, kv_width), jnp.bfloat16),
        ),
        in_specs=[apart] * 5 + [smem] + [apart] * 2,
        out_specs=(held,) * 3,
        scratch_shapes=[
            pltpu.VMEM((4, shard, group_cols), jnp.bfloat16),
            pltpu.VMEM((shard, group_cols), jnp.bfloat16),
            pltpu.VMEM((shard, width), jnp.bfloat16),
            pltpu.VMEM((width,), jnp.float32),
            pltpu.SMEM((1, n), jnp.int32),
            pltpu.VMEM((n, 2, shard, HD), jnp.bfloat16),
            pltpu.VMEM((2, shard, HD), jnp.bfloat16),
            pltpu.VMEM((n, 2, 2, shard // n, HD), jnp.bfloat16),
            pltpu.VMEM((n, 2, 2, shard // n, HD), jnp.bfloat16),
            slab, slab, slab, slab, slab,
            pltpu.VMEM((4, 2, group_cols, width), jnp.bfloat16),
            pltpu.VMEM((group_cols // HD, 4, shard, HD), jnp.float32),
            pltpu.VMEM((group_cols // HD, 4, shard, LANES), jnp.float32),
            pltpu.VMEM((2, group_cols // HD, 2 * shard, HD), jnp.bfloat16),
            pltpu.VMEM((2, chunks, ROWS, group_cols), jnp.bfloat16),
            pltpu.VMEM((chunks, ROWS, group_cols), jnp.bfloat16),
            pltpu.VMEM((2, chunks, ROWS, group_cols), jnp.bfloat16),
            half, half, half, half, half, half,
            pltpu.VMEM((2, shard, width), jnp.float32),
            pltpu.VMEM((shard, width), jnp.float32),
            pltpu.VMEM((shard, LANES), jnp.float32),
            pltpu.VMEM((8, shard), jnp.float32),
            pltpu.VMEM((4, 8, shard), jnp.float32),
            pltpu.SemaphoreType.DMA((9,)),
            one,
            one,
            one,
            pltpu.SemaphoreType.DMA((3,)),
            one,
            pltpu.SemaphoreType.DMA((n - 2, 2)),
            one,
            one,
            one,
            one,
            one,
            one,
            one,
            one,
            one,
            one,
            one,
            one,
            pltpu.SemaphoreType.DMA((chunks,)),
            pltpu.SemaphoreType.DMA((3,)),
            pltpu.SemaphoreType.DMA((2, chunks)),
            one,
            one,
            one,
            pltpu.SemaphoreType.REGULAR,
        ],
        compiler_params=pltpu.CompilerParams(
            collective_id=0, has_side_effects=True, vmem_limit_bytes=62 * 1024 * 1024
        ),
    )(
        queries[0], key_rows[0], value_rows[0], residual[0], post_scale, lengths, owners,
        out_weight,
    )
    made = (hidden, ck, cv)
    hidden, ck, cv = pl.pallas_call(
        put_out,
        out_shape=tuple(jax.ShapeDtypeStruct(a.shape, a.dtype) for a in made),
        in_specs=[apart] * len(made),
        out_specs=(apart,) * len(made),
        scratch_shapes=[pltpu.SemaphoreType.DMA((len(made),))],
    )(*(pltpu.with_memory_space_constraint(a, pltpu.VMEM) for a in made))
    return hidden[None], ck[None], cv[None]


def solution(mesh):
    placed = (
        P(None, "seq", "tp"),
        P(None, "seq", "tp"),
        P(None, "seq", "tp"),
        P(None, "seq", "tp"),
        P("tp", None),
        P("tp"),
        P(),
        P(),
    )
    return jax.shard_map(
        local,
        mesh=mesh,
        in_specs=placed,
        out_specs=(P(None, "seq", "tp"), P(None, "seq", "tp"), P(None, "seq", "tp")),
        check_vma=False,
    )
```

```python
import functools

import jax
import jax.numpy as jnp
from jax import lax
from jax.experimental import pallas as pl
from jax.experimental.pallas import tpu as pltpu
from jax.sharding import PartitionSpec as P

D = 3584
HD = 256
WINDOW = 4096
MESH = pl.DeviceIdType.MESH
LOG2E = 1.4426950408889634
ROWS = 32
LANES = 128


soft_cap = 50.0
norm_eps = 1e-06


def shifted(x, axis, by):
    peers = lax.axis_size(axis)
    pairs = [(i, i + by) for i in range(peers) if 0 <= i + by < peers]
    return lax.ppermute(x, axis, pairs)


def attend_block(grouped, block_keys, block_values, query_pos, key_pos, state_pair):
    numerator, denominator = state_pair
    seq_count, query_count, kv_local, group_size, head_size = grouped.shape
    keyed_rows = block_keys.reshape(seq_count, block_keys.shape[1], kv_local, head_size)
    valued_rows = block_values.reshape(seq_count, block_values.shape[1], kv_local, head_size)
    scores = jnp.einsum(
        "sqhgd,skhd->shgqk", grouped, keyed_rows, preferred_element_type=jnp.float32
    ) * head_size ** (-0.5)
    capped = soft_cap * jnp.tanh(scores / soft_cap)
    spread = query_pos[:, None] - key_pos[None, :]
    live_mask = (spread >= 0) & (spread < WINDOW) & (key_pos[None, :] >= 0)
    weights = jnp.where(live_mask, jnp.exp(capped), jnp.zeros_like(capped))
    denominator = denominator + jnp.sum(weights, axis=-1)
    numerator = numerator + jnp.einsum(
        "shgqk,skhd->sqhgd",
        weights.astype(jnp.bfloat16),
        valued_rows,
        preferred_element_type=jnp.float32,
    )
    return (numerator, denominator)


def reorder_blocks(blocked, ordering):
    return blocked[ordering]


def local(queries, key_rows, value_rows, residual, out_weight, post_scale, lengths, owners):
    seq_count, shard_len, query_width = queries.shape
    seq_size = lax.axis_size("seq")
    if (
        seq_count == 1 and lax.axis_size("tp") == 4 and seq_size % 2 == 0 and seq_size >= 8
        and seq_size * shard_len <= WINDOW and key_rows.shape[2] == 2 * HD
        and shard_len % LANES == 0
    ):
        return fused(
            seq_size, queries, key_rows, value_rows, residual, out_weight, post_scale, lengths,
            owners,
        )
    kv_width = key_rows.shape[2]
    kv_local = kv_width // HD
    group_size = query_width // kv_width
    grouped = queries.reshape(seq_count, shard_len, kv_local, group_size, HD)
    position = lax.axis_index("seq")
    seq_devices = lax.axis_size("seq")
    offsets = jnp.arange(shard_len, dtype=jnp.int32)
    query_pos = position * shard_len + offsets
    numerator = jnp.zeros((seq_count, shard_len, kv_local, group_size, HD), jnp.float32)
    denominator = jnp.zeros((seq_count, kv_local, group_size, shard_len), jnp.float32)
    state_pair = attend_block(
        grouped, key_rows, value_rows, query_pos, query_pos, (numerator, denominator)
    )
    hop_count = min(WINDOW // shard_len, seq_devices - 1)
    arrived = []
    current = (key_rows, value_rows)
    for hop_index in range(1, hop_count + 1):
        current = shifted((current[0], current[1]), "seq", 1)
        arrived.append((hop_index, current))
        if len(arrived) == 2 or hop_index == hop_count:
            ordered = arrived[::-1]
            block_keys = jnp.concatenate([member[1][0] for member in ordered], axis=1)
            block_values = jnp.concatenate([member[1][1] for member in ordered], axis=1)
            block_pos = jnp.concatenate(
                [(position - member[0]) * shard_len + offsets for member in ordered]
            )
            state_pair = attend_block(
                grouped, block_keys, block_values, query_pos, block_pos, state_pair
            )
            arrived = []
    numerator, denominator = state_pair
    attended = (numerator / jnp.transpose(denominator, (0, 3, 1, 2))[..., None]).astype(
        jnp.bfloat16
    )
    partial_value = jnp.dot(
        attended.reshape(seq_count * shard_len, query_width),
        out_weight,
        preferred_element_type=jnp.float32,
    )
    partial_value = partial_value.reshape(seq_count, shard_len, out_weight.shape[1])
    branch = lax.psum_scatter(partial_value, "tp", scatter_dimension=2, tiled=True)
    squares = lax.psum(jnp.sum(branch * branch, axis=-1), "tp")
    normed = branch * lax.rsqrt(squares / D + norm_eps)[..., None] * post_scale
    hidden_out = (residual.astype(jnp.float32) + normed).astype(jnp.bfloat16)
    block_rows = shard_len // seq_devices
    slot_span = WINDOW // shard_len
    live_rows = (query_pos[None, :] >= lengths[:, None] - WINDOW) & (
        query_pos[None, :] < lengths[:, None]
    )
    kept_keys = jnp.where(live_rows[..., None], key_rows, jnp.zeros_like(key_rows))
    kept_values = jnp.where(live_rows[..., None], value_rows, jnp.zeros_like(value_rows))
    devices = jnp.arange(seq_devices, dtype=jnp.int32)
    matches = owners[:, :, None] == devices[None, None, :]
    inverse = jnp.sum(
        jnp.where(matches, devices[None, :, None], jnp.zeros_like(devices)[None, :, None]), axis=1
    )
    outgoing_keys = jax.vmap(reorder_blocks)(
        kept_keys.reshape(seq_count, seq_devices, block_rows, kv_width), inverse
    )
    outgoing_values = jax.vmap(reorder_blocks)(
        kept_values.reshape(seq_count, seq_devices, block_rows, kv_width), inverse
    )
    incoming = (
        lax.all_to_all(outgoing_keys, "seq", split_axis=1, concat_axis=1, tiled=True),
        lax.all_to_all(outgoing_values, "seq", split_axis=1, concat_axis=1, tiled=True),
    )
    selector = (
        devices[None, :] % slot_span == jnp.arange(slot_span, dtype=jnp.int32)[:, None]
    ).astype(jnp.bfloat16)
    cache_keys = (
        jnp.einsum("md,sdbf->smbf", selector, incoming[0], preferred_element_type=jnp.float32)
        .astype(jnp.bfloat16)
        .reshape(seq_count, slot_span * block_rows, kv_width)
    )
    cache_values = (
        jnp.einsum("md,sdbf->smbf", selector, incoming[1], preferred_element_type=jnp.float32)
        .astype(jnp.bfloat16)
        .reshape(seq_count, slot_span * block_rows, kv_width)
    )
    return (hidden_out, cache_keys, cache_values)


def layer_kernel(
    n, q_hbm, k_hbm, v_hbm, res_hbm, scale_hbm, len_ref, own_hbm, w_ref,
    hid_ref, ck_ref, cv_ref,
    qall, qpart, res_ref, scale_ref, own_ref, kv, other,
    down_out, down_in, pair_out, pair_in, line_out, line_in, skew_out,
    wbuf, acc, den, rounded, att, att_out, lent_out,
    to_sib, to_x, to_sib2, from_sib, from_x, from_sib2, early, total, folds, sq_out, sq_in,
    in_sem, w_sem, y_send, yq_send, y_recv, z_send, z_recv, lend_recv, q_send, q_recv, lent_send,
    down_send, down_recv, pair_send, pair_recv, line_send, line_recv, skew_send, att_send, att_recv,
    rs_send, rs_recv, sib2_recv, sq_send, sq_recv, turn, lower, upper,
):
    nz = n // 2
    top = nz - 1
    me = lax.axis_index("seq")
    t = lax.axis_index("tp")
    z, y = me // 2, me % 2
    x, c = t // 2, t % 2
    sib = x * 2 + (1 - c)
    across = (1 - x) * 2 + c
    diagonal = (1 - x) * 2 + (1 - c)
    partner = z * 2 + (1 - y)
    shard = kv.shape[2]
    width = res_ref.shape[1]
    group_cols = qpart.shape[1]
    group = group_cols // HD
    block_rows = shard // n
    chunks = shard // ROWS
    merge = LANES // ROWS
    lends = (c == 1) & (z == top)
    hosts = (c == 1) & (z == top - 1)
    takes_kv = (z < top) | (c == 0)
    sends_kv = (z < top - 1) | ((z < top) & (c == 0))

    frees = (c == 0) & (z == top - 2)
    defers = (c == 1) & (z == top - 2)

    def half(ref, which, cols):
        return ref.at[:, pl.ds(pl.multiple_of(which * cols, cols), cols)]

    loads = [
        pltpu.make_async_copy(src, dst, in_sem.at[i])
        for i, (src, dst) in enumerate(
            (
                (half(k_hbm, 1 - y, HD), other.at[0]), (half(v_hbm, 1 - y, HD), other.at[1]),
                (half(k_hbm, y, HD), kv.at[me, 0]), (half(v_hbm, y, HD), kv.at[me, 1]),
                (half(q_hbm, 1 - y, group_cols), qpart), (half(q_hbm, y, group_cols), qall.at[y]),
                (own_hbm, own_ref), (res_hbm, res_ref), (scale_hbm, scale_ref),
            )
        )
    ]
    for load in loads[:7]:
        load.start()

    barrier = pltpu.get_barrier_semaphore()
    for peer in (sib, across, diagonal):
        pl.semaphore_signal(barrier, inc=1, device_id={"tp": peer}, device_id_type=MESH)
    pl.semaphore_signal(barrier, inc=1, device_id={"seq": partner}, device_id_type=MESH)
    for there, peer in ((z < top, me + 2), (z > 0, me - 2)):

        @pl.when(there)
        def _():
            pl.semaphore_signal(barrier, inc=1, device_id={"seq": peer}, device_id_type=MESH)

    def clear(s, carry):
        acc[s] = jnp.zeros(acc.shape[1:], jnp.float32)
        den[s] = jnp.zeros(den.shape[1:], jnp.float32)
        return carry

    lax.fori_loop(0, acc.shape[0], clear, 0)
    pl.semaphore_wait(barrier, 4 + jnp.where(z < top, 1, 0) + jnp.where(z > 0, 1, 0))

    def remote(src, dst, send, recv, to):
        return pltpu.make_async_remote_copy(
            src_ref=src, dst_ref=dst, send_sem=send, recv_sem=recv, device_id=to,
            device_id_type=MESH,
        )

    def settle(ref, sem):
        pltpu.make_async_copy(ref, ref, sem.at[0]).wait()

    def y_copy(h, origin):
        return remote(
            other.at[h], kv.at[origin, h], y_send.at[0], y_recv.at[h], {"seq": partner}
        )

    def yq_copy(slot):
        return remote(qpart, qall.at[slot], yq_send.at[0], y_recv.at[2], {"seq": partner})

    def z_copy(origin, h):
        return remote(
            kv.at[origin, h], kv.at[origin, h], z_send.at[0], z_recv.at[origin, h],
            {"seq": me + 2},
        )

    def lend_copy(yq):
        return remote(
            qall.at[yq], qall.at[2 + yq], q_send.at[0], q_recv.at[0], {"seq": me - 2}
        )

    def lend_kv(origin, h):
        return remote(
            kv.at[origin, h], kv.at[origin, h], z_send.at[0], lend_recv.at[0],
            {"seq": me - 2},
        )

    def w_copy(f, g):
        return pltpu.make_async_copy(
            w_ref.at[pl.ds(g * group_cols, group_cols), pl.ds(f * width, width)],
            wbuf.at[f, g], w_sem.at[0],
        )

    for h in (0, 1):
        loads[2 + h].wait()
        pl.when(sends_kv)(z_copy(me, h).start)
    for load in (loads[0], loads[1], loads[4], loads[5]):
        load.wait()

    @pl.when(z == top)
    def _():
        yq_copy(y).start()
        for h in (0, 1):
            y_copy(h, me).start()

    @pl.when(z < top)
    def _():
        for h in (0, 1):
            y_copy(h, me).start()
        yq_copy(y).start()

    @pl.when(lends)
    def _():
        lend_copy(y).start()
        for h in (0, 1):
            lend_kv(me, h).start()

    loads[6].wait()
    for f in range(4):
        for g in (0, 1):
            w_copy(f, g).start()
    for load in loads[7:]:
        load.start()

    @pl.when(z > 0)
    def _():
        pl.semaphore_wait(lower, 1)

    @pl.when(z < top)
    def _():
        pl.semaphore_signal(lower, inc=1, device_id={"seq": me + 2}, device_id_type=MESH)

    @pl.when(lends)
    def _():
        pl.semaphore_signal(upper, inc=1, device_id={"seq": me - 2}, device_id_type=MESH)

    def owned(device):
        block = own_ref[0, 0] * 0
        for b in range(n):
            block = block + jnp.where(own_ref[0, b] == device, b, 0)
        return jnp.full((block_rows, HD), block, jnp.int32)

    def select(ref, lead, chosen):
        got = jnp.zeros(chosen.shape, jnp.float32)
        for b in range(n):
            rows = ref[(*lead, slice(b * block_rows, (b + 1) * block_rows))]
            got = jnp.where(chosen == b, rows.astype(jnp.float32), got)
        return got.astype(jnp.bfloat16)

    def down_copy(to, slot):
        return remote(
            down_out.at[to], down_in.at[slot], down_send.at[0], down_recv.at[0], {"seq": to}
        )

    def stage(to, carry):
        chosen = owned(to)
        for h in (0, 1):
            down_out[to, h, y] = select(kv, (me, h), chosen)
            down_out[to, h, 1 - y] = select(other, (h,), chosen)
        return carry

    def post(to, carry):
        down_copy(to, me).start()
        return carry

    lax.fori_loop(0, 2 * z, stage, 0)

    def pair_copy(zo):
        return remote(
            pair_out.at[zo], pair_in.at[zo], pair_send.at[0], pair_recv.at[0], {"seq": partner}
        )

    def line_copy(zo):
        return remote(
            line_out.at[zo], line_in.at[zo], line_send.at[0], line_recv.at[0], {"seq": me + 2}
        )

    def skew_copy(zo):
        return remote(
            skew_out.at[zo], pair_in.at[zo], skew_send.at[0], pair_recv.at[0],
            {"seq": partner + 2},
        )

    def gather(zo, device, out):
        chosen = owned(device)
        for yo in (0, 1):
            for h in (0, 1):
                out[zo, yo, h] = select(kv, (2 * zo + yo, h), chosen)

    def pass_cache(zo):
        @pl.when((zo == z) | takes_kv)
        def _():
            gather(zo, partner, pair_out)
            pair_copy(zo).start()

    def lift_cache(zo):
        gather(zo, me + 2, line_out)
        line_copy(zo).start()
        gather(zo, partner + 2, skew_out)
        skew_copy(zo).start()

    @pl.when(lends)
    def _():
        yq_copy(1 - y).wait_recv()
        lend_copy(1 - y).start()

    for h in (0, 1):
        y_copy(h, partner).wait_recv()
        pl.when(sends_kv)(z_copy(partner, h).start)
        pl.when(lends)(lend_kv(partner, h).start)
    lax.fori_loop(0, 2 * z, post, 0)

    @pl.when(hosts)
    def _():
        pl.semaphore_wait(upper, 1)
        lift_cache(z)

    def take(origin, h):
        z_copy(origin, h).wait_recv()
        held_back = defers & (origin == 1 - y)
        pl.when(sends_kv & jnp.logical_not(held_back))(z_copy(origin, h).start)

    @pl.when((z > 0) & takes_kv)
    def _():
        for origin in (me - 2, partner - 2):
            for h in (0, 1):
                take(origin, h)

    @pl.when(hosts & (z > 1))
    def _():
        lift_cache(z - 1)

    @pl.when(jnp.logical_not(lends))
    def _():
        yq_copy(1 - y).wait_recv()

    def attend(base, origin, above):
        pair = pl.ds(base, 2)
        for hh in range(group):
            stacked = qall[pair, :, hh * HD : (hh + 1) * HD].reshape(2 * shard, HD)
            scores = lax.dot_general(
                stacked, kv[origin, 0], (((1,), (1,)), ((), ())),
                preferred_element_type=jnp.float32,
            )
            w = jnp.exp2(jnp.tanh(scores * (HD ** (-0.5) / soft_cap)) * (soft_cap * LOG2E))
            if above is not None:
                keep = lax.broadcasted_iota(jnp.int32, w.shape, 0) >= above + (
                    lax.broadcasted_iota(jnp.int32, w.shape, 1)
                )
                w = jnp.where(keep, w, 0.0)
            folded = w[:, :LANES]
            for i in range(1, w.shape[1] // LANES):
                folded = folded + w[:, i * LANES : (i + 1) * LANES]
            den[hh, pair] += folded.reshape(2, shard, LANES)
            acc[hh, pair] += jnp.dot(
                w.astype(jnp.bfloat16), kv[origin, 1], preferred_element_type=jnp.float32
            ).reshape(2, shard, HD)

    def weigh(i, origin):
        pair = pl.ds(2 * i, 2)
        for hh in range(group):
            stacked = qall[pair, :, hh * HD : (hh + 1) * HD].reshape(2 * shard, HD)
            scores = lax.dot_general(
                stacked, kv[origin, 0], (((1,), (1,)), ((), ())),
                preferred_element_type=jnp.float32,
            )
            w = jnp.exp2(jnp.tanh(scores * (HD ** (-0.5) / soft_cap)) * (soft_cap * LOG2E))
            folded = w[:, :LANES]
            for j in range(1, w.shape[1] // LANES):
                folded = folded + w[:, j * LANES : (j + 1) * LANES]
            den[hh, pair] += folded.reshape(2, shard, LANES)
            rounded[i, hh] = w.astype(jnp.bfloat16)

    def mix(i, origin):
        pair = pl.ds(2 * i, 2)
        for hh in range(group):
            acc[hh, pair] += jnp.dot(
                rounded[i, hh], kv[origin, 1], preferred_element_type=jnp.float32
            ).reshape(2, shard, HD)

    def invert():
        def one(i, carry):
            pair = pl.ds(2 * i, 2)
            for hh in range(group):
                whole = den[hh, pair].reshape(2 * shard, LANES)
                inverse = 1.0 / jnp.sum(whole, axis=-1, keepdims=True)
                den[hh, pair] = jnp.broadcast_to(inverse, whole.shape).reshape(2, shard, LANES)
            return carry

        lax.fori_loop(0, jnp.where(hosts, 2, 1), one, 0)

    def own_slab(base, slab):
        def diagonal_block(i, carry):
            attend(base, 2 * slab + i, i * shard)
            return carry

        lax.fori_loop(0, 2, diagonal_block, 0)

    pl.when(jnp.logical_not(lends))(functools.partial(own_slab, 0, z))
    @pl.when(hosts)
    def _():
        settle(qall.at[2:], q_recv)

        def one(i, carry):
            attend(2, 2 * z + i, None)
            return carry

        lax.fori_loop(0, 2, one, 0)

    def rows_of(r):
        return pl.ds(pl.multiple_of(r * ROWS, ROWS), ROWS)

    def att_copy(r, g):
        return remote(
            att_out.at[r], att.at[g, r], att_send.at[0], att_recv.at[r], {"seq": partner}
        )

    def lent_copy(yq, r, g):
        return remote(
            lent_out.at[yq, r], att.at[g, r], lent_send.at[0], att_recv.at[r],
            {"seq": 2 * top + yq},
        )

    def finish(s, r, out, lead):
        for hh in range(group):
            for i in range(HD // LANES):
                cols = slice(i * LANES, (i + 1) * LANES)
                out[(*lead, slice(None), slice(hh * HD + i * LANES, hh * HD + (i + 1) * LANES))] = (
                    acc[hh, s, rows_of(r), cols] * den[hh, s, rows_of(r), :]
                ).astype(jnp.bfloat16)

    def give(r, carry):
        for yq in (1 - y, y):
            finish(2 + yq, r, lent_out, (yq, r))
            lent_copy(yq, r, y).start()
        return carry

    pairs = jnp.where(hosts, 2, 1)

    def phase(d, carry):
        @pl.when(z - d + 1 >= 1)
        def _():
            pass_cache(z - d + 1)

        @pl.when(hosts & (d > 2) & (z - d + 1 >= 1))
        def _():
            lift_cache(z - d + 1)

        @pl.when(hosts & (d == jnp.minimum(2, z)))
        def _():
            settle(kv.at[2 * top :], lend_recv)
            own_slab(2, top)

        def side(j, carry):
            @pl.when((z - d >= 0) & takes_kv)
            def _():
                origin = 2 * (z - d) + jnp.where(j == 0, y, 1 - y)
                for h, work in enumerate((weigh, mix)):
                    pl.when(d > 1)(functools.partial(take, origin, h))

                    def one(i, carry):
                        which = pairs - 1 - i
                        work(which, origin)
                        if h == 1:

                            @pl.when((which == 1) & (d == z) & (j == 1))
                            def _():
                                lax.fori_loop(0, chunks, give, 0)

                        return carry

                    lax.fori_loop(0, pairs, one, 0)
                    if h == 0:
                        pl.when((d == z) & (j == 1))(invert)

            return carry

        lax.fori_loop(0, 2, side, 0)
        return carry

    lax.fori_loop(1, nz, phase, 0)

    pl.when(z == 0)(invert)

    @pl.when(frees)
    def _():
        settle(kv.at[: 2 * top - 2], z_send)
        pl.semaphore_signal(turn, inc=1, device_id={"tp": sib}, device_id_type=MESH)

    @pl.when(defers)
    def _():
        pl.semaphore_wait(turn, 1)
        for h in (0, 1):
            z_copy(1 - y, h).start()

    def away(r, carry):
        finish(1 - y, r, att_out, (r,))
        att_copy(r, y).start()
        return carry

    def home(r, carry):
        finish(y, r, att, (y, r))
        return carry

    @pl.when(jnp.logical_not(lends))
    def _():
        lax.fori_loop(0, chunks, away, 0)
        lax.fori_loop(0, chunks, home, 0)

    def rs_copy(kind, r, src, dst, recv, to):
        return remote(src.at[r], dst.at[r], rs_send.at[kind], recv, {"tp": to})

    def sib_copy(r):
        return rs_copy(0, r, to_sib, from_sib, rs_recv.at[0, r], sib)

    def x_copy(r):
        return rs_copy(1, r, to_x, from_x, rs_recv.at[1, r], across)

    def sib2_copy(r):
        return rs_copy(2, r, to_sib2, from_sib2, sib2_recv.at[0], sib)

    def product(rows, f, g):
        return jnp.dot(rows, wbuf[f, g], preferred_element_type=jnp.float32)

    def part(f, r):
        some = pl.ds(merge * r, merge)
        rows = [att[g, some].reshape(LANES, group_cols) for g in (0, 1)]
        return product(rows[0], f, 0) + product(rows[1], f, 1)

    settle(wbuf, w_sem)

    sent = (diagonal, across)

    @pl.when(jnp.logical_not(lends))
    def _():
        for i, f in enumerate(sent):
            early[i] = product(att[y].reshape(shard, group_cols), f, y)

    def send_sib(r):
        pl.when(jnp.logical_not(lends))(att_copy(r, 1 - y).wait_recv)

        @pl.when(lends)
        def _():
            both_heads = att.at[:, r]
            pltpu.make_async_copy(both_heads, both_heads, att_recv.at[r]).wait()
            early[0, rows_of(r), :] = product(att[y, r], diagonal, y)

        to_sib[r] = (early[0, rows_of(r), :] + product(att[1 - y, r], diagonal, 1 - y)).astype(
            jnp.bfloat16
        )
        sib_copy(r).start()

    def send_x(r):
        @pl.when(lends)
        def _():
            early[1, rows_of(r), :] = product(att[y, r], across, y)

        mine = early[1, rows_of(r), :] + product(att[1 - y, r], across, 1 - y)
        sib_copy(r).wait_recv()
        to_x[r] = (mine + from_sib[r].astype(jnp.float32)).astype(jnp.bfloat16)
        x_copy(r).start()

    def both(r, carry):
        pl.when(r < chunks)(functools.partial(send_sib, r))
        pl.when(r > 0)(functools.partial(send_x, r - 1))
        return carry

    def third(r, carry):
        some = pl.ds(merge * r, merge)
        to_sib2[some] = part(sib, r).astype(jnp.bfloat16).reshape(merge, ROWS, width)
        for i in range(merge):
            sib2_copy(merge * r + i).start()
        return carry

    def fourth(r, carry):
        rows = pl.ds(pl.multiple_of(r * LANES, LANES), LANES)
        total[rows, :] = part(t, r)
        return carry

    lax.fori_loop(0, chunks + 1, both, 0)

    pass_cache(0)
    pl.when(hosts)(functools.partial(lift_cache, 0))

    for step in (third, fourth):
        lax.fori_loop(0, chunks // merge, step, 0)

    mine_blocks = owned(me)
    local_row = lax.broadcasted_iota(jnp.int32, mine_blocks.shape, 0)
    bound = jnp.full(mine_blocks.shape, len_ref[0], jnp.int32)

    for slab in range(nz):

        @pl.when(z == slab)
        def _():
            settle(pair_in.at[: slab + 1], pair_recv)
            if slab < top:
                settle(down_in.at[2 * slab + 2 :], down_recv)

    @pl.when(lends)
    def _():
        settle(line_in.at[:top], line_recv)

    def cache(zo, carry):
        far = lends & (zo < top)

        for yo in (0, 1):
            origin = 2 * zo + yo
            pos = local_row + mine_blocks * block_rows + origin * shard
            live = (pos < bound) & (pos >= bound - WINDOW)
            rows = pl.ds(pl.multiple_of(origin * block_rows, block_rows), block_rows)

            for h, out in enumerate((ck_ref, cv_ref)):

                def put(g, value):
                    cols = pl.ds(pl.multiple_of(g * HD, HD), HD)
                    out[rows, cols] = jnp.where(live, value.astype(jnp.float32), 0.0).astype(
                        jnp.bfloat16
                    )

                @pl.when(zo > z)
                def _():
                    for g in (0, 1):
                        put(g, down_in[origin, h, g])

                @pl.when(zo <= z)
                def _():
                    put(1 - y, pair_in[zo, yo, h])

                @pl.when((zo <= z) & jnp.logical_not(far))
                def _():
                    put(y, select(kv, (origin, h), mine_blocks))

                @pl.when(far)
                def _():
                    put(y, line_in[zo, yo, h])

        return carry

    lax.fori_loop(0, nz, cache, 0)
    rest = ck_ref.shape[0] - n * block_rows
    if rest:
        for out in (ck_ref, cv_ref):
            out[n * block_rows :, :] = jnp.zeros((rest, 2 * HD), jnp.bfloat16)
    settle(from_sib2, sib2_recv)
    for r in range(chunks):
        x_copy(r).wait_recv()
        rows = slice(r * ROWS, (r + 1) * ROWS)
        branch = total[rows, :] + from_sib2[r].astype(jnp.float32) + from_x[r].astype(jnp.float32)
        total[rows, :] = branch
        squared = branch * branch
        folded = squared[:, :LANES]
        for i in range(1, width // LANES):
            folded = folded + squared[:, i * LANES : (i + 1) * LANES]
        folds[rows, :] = folded
        if (r + 1) * ROWS % LANES == 0:
            rows = slice((r + 1) * ROWS - LANES, (r + 1) * ROWS)
            line = jnp.sum(folds[rows, :].T, axis=0, keepdims=True)
            sq_out[:, rows] = jnp.broadcast_to(line, (8, LANES))

    def sq_copy(i, to, slot):
        return pltpu.make_async_remote_copy(
            src_ref=sq_out, dst_ref=sq_in.at[slot], send_sem=sq_send.at[0],
            recv_sem=sq_recv.at[0], device_id={"tp": to}, device_id_type=MESH,
        )

    peers = (sib, across, diagonal)
    for i, peer in enumerate(peers):
        sq_copy(i, peer, t).start()
    squares = sq_out[...]
    settle(sq_in.at[:3], sq_recv)
    for i, peer in enumerate(peers):
        squares = squares + sq_in[peer]
    loads[7].wait()
    loads[8].wait()
    factor = lax.rsqrt(squares / D + norm_eps)
    for r in range(shard // LANES):
        rows = slice(r * LANES, (r + 1) * LANES)
        spread = jnp.broadcast_to(factor[:1, rows], (LANES, LANES)).T
        for i in range(width // LANES):
            cols = slice(i * LANES, (i + 1) * LANES)
            normed = total[rows, cols] * spread * scale_ref[cols].reshape(1, LANES)
            hid_ref[rows, cols] = (res_ref[rows, cols].astype(jnp.float32) + normed).astype(
                jnp.bfloat16
            )

    settle(sq_in.at[:3], sq_send)
    for kind, sent_rows in enumerate((to_sib, to_x, to_sib2)):
        pltpu.make_async_copy(sent_rows, sent_rows, rs_send.at[kind]).wait()
    settle(other, y_send)
    settle(qpart, yq_send)
    for slab in range(nz):

        @pl.when((z == slab) & sends_kv & jnp.logical_not(frees))
        def _():
            settle(kv.at[: 2 * slab + 2], z_send)

        @pl.when((z == slab) & takes_kv)
        def _():
            settle(pair_out.at[: slab + 1], pair_send)

        if slab:

            @pl.when(z == slab)
            def _():
                settle(down_out.at[: 2 * slab], down_send)

    @pl.when(lends)
    def _():
        settle(qall.at[:2], q_send)
        settle(kv.at[2 * top :], z_send)
        settle(pair_out.at[top:], pair_send)

    @pl.when(jnp.logical_not(lends))
    def _():
        settle(att_out, att_send)

    @pl.when(hosts)
    def _():
        settle(lent_out, lent_send)
        settle(line_out.at[:top], line_send)
        settle(skew_out.at[:top], skew_send)


def put_out(*refs):
    count = (len(refs) - 1) // 2
    copies = [
        pltpu.make_async_copy(refs[i], refs[count + i], refs[-1].at[i]) for i in range(count)
    ]
    for copy in copies:
        copy.start()
    for copy in copies:
        copy.wait()


def fused(n, queries, key_rows, value_rows, residual, out_weight, post_scale, lengths, owners):
    shard, q_width = queries.shape[1:]
    kv_width = key_rows.shape[2]
    width = residual.shape[2]
    chunks = shard // ROWS
    cache_rows = WINDOW // n
    smem = pl.BlockSpec(memory_space=pltpu.SMEM)
    apart = pl.BlockSpec(memory_space=pl.ANY)
    held = pl.BlockSpec(memory_space=pltpu.VMEM)
    one = pltpu.SemaphoreType.DMA((1,))
    group_cols = q_width * HD // kv_width
    slab = pltpu.VMEM((n // 2, 2, 2, shard // n, HD), jnp.bfloat16)
    half = pltpu.VMEM((chunks, ROWS, width), jnp.bfloat16)
    hidden, ck, cv = pl.pallas_call(
        functools.partial(layer_kernel, n),
        out_shape=(
            pltpu.VMEM((shard, width), jnp.bfloat16),
            pltpu.VMEM((cache_rows, kv_width), jnp.bfloat16),
            pltpu.VMEM((cache_rows, kv_width), jnp.bfloat16),
        ),
        in_specs=[apart] * 5 + [smem] + [apart] * 2,
        out_specs=(held,) * 3,
        scratch_shapes=[
            pltpu.VMEM((4, shard, group_cols), jnp.bfloat16),
            pltpu.VMEM((shard, group_cols), jnp.bfloat16),
            pltpu.VMEM((shard, width), jnp.bfloat16),
            pltpu.VMEM((width,), jnp.float32),
            pltpu.SMEM((1, n), jnp.int32),
            pltpu.VMEM((n, 2, shard, HD), jnp.bfloat16),
            pltpu.VMEM((2, shard, HD), jnp.bfloat16),
            pltpu.VMEM((n, 2, 2, shard // n, HD), jnp.bfloat16),
            pltpu.VMEM((n, 2, 2, shard // n, HD), jnp.bfloat16),
            slab, slab, slab, slab, slab,
            pltpu.VMEM((4, 2, group_cols, width), jnp.bfloat16),
            pltpu.VMEM((group_cols // HD, 4, shard, HD), jnp.float32),
            pltpu.VMEM((group_cols // HD, 4, shard, LANES), jnp.float32),
            pltpu.VMEM((2, group_cols // HD, 2 * shard, HD), jnp.bfloat16),
            pltpu.VMEM((2, chunks, ROWS, group_cols), jnp.bfloat16),
            pltpu.VMEM((chunks, ROWS, group_cols), jnp.bfloat16),
            pltpu.VMEM((2, chunks, ROWS, group_cols), jnp.bfloat16),
            half, half, half, half, half, half,
            pltpu.VMEM((2, shard, width), jnp.float32),
            pltpu.VMEM((shard, width), jnp.float32),
            pltpu.VMEM((shard, LANES), jnp.float32),
            pltpu.VMEM((8, shard), jnp.float32),
            pltpu.VMEM((4, 8, shard), jnp.float32),
            pltpu.SemaphoreType.DMA((9,)),
            one,
            one,
            one,
            pltpu.SemaphoreType.DMA((3,)),
            one,
            pltpu.SemaphoreType.DMA((n - 2, 2)),
            one,
            one,
            one,
            one,
            one,
            one,
            one,
            one,
            one,
            one,
            one,
            one,
            pltpu.SemaphoreType.DMA((chunks,)),
            pltpu.SemaphoreType.DMA((3,)),
            pltpu.SemaphoreType.DMA((2, chunks)),
            one,
            one,
            one,
            pltpu.SemaphoreType.REGULAR,
            pltpu.SemaphoreType.REGULAR,
            pltpu.SemaphoreType.REGULAR,
        ],
        compiler_params=pltpu.CompilerParams(
            collective_id=0, has_side_effects=True, vmem_limit_bytes=62 * 1024 * 1024
        ),
    )(
        queries[0], key_rows[0], value_rows[0], residual[0], post_scale, lengths, owners,
        out_weight,
    )
    made = (hidden, ck, cv)
    hidden, ck, cv = pl.pallas_call(
        put_out,
        out_shape=tuple(jax.ShapeDtypeStruct(a.shape, a.dtype) for a in made),
        in_specs=[apart] * len(made),
        out_specs=(apart,) * len(made),
        scratch_shapes=[pltpu.SemaphoreType.DMA((len(made),))],
    )(*(pltpu.with_memory_space_constraint(a, pltpu.VMEM) for a in made))
    return hidden[None], ck[None], cv[None]


def solution(mesh):
    placed = (
        P(None, "seq", "tp"),
        P(None, "seq", "tp"),
        P(None, "seq", "tp"),
        P(None, "seq", "tp"),
        P("tp", None),
        P("tp"),
        P(),
        P(),
    )
    return jax.shard_map(
        local,
        mesh=mesh,
        in_specs=placed,
        out_specs=(P(None, "seq", "tp"), P(None, "seq", "tp"), P(None, "seq", "tp")),
        check_vma=False,
    )
```

```python
import functools

import jax
import jax.numpy as jnp
from jax import lax
from jax.experimental import pallas as pl
from jax.experimental.pallas import tpu as pltpu
from jax.sharding import PartitionSpec as P

D = 3584
HD = 256
WINDOW = 4096
MESH = pl.DeviceIdType.MESH
LOG2E = 1.4426950408889634
ROWS = 32
LANES = 128
PIECES = 4


soft_cap = 50.0
norm_eps = 1e-06


def shifted(x, axis, by):
    peers = lax.axis_size(axis)
    pairs = [(i, i + by) for i in range(peers) if 0 <= i + by < peers]
    return lax.ppermute(x, axis, pairs)


def attend_block(grouped, block_keys, block_values, query_pos, key_pos, state_pair):
    numerator, denominator = state_pair
    seq_count, query_count, kv_local, group_size, head_size = grouped.shape
    keyed_rows = block_keys.reshape(seq_count, block_keys.shape[1], kv_local, head_size)
    valued_rows = block_values.reshape(seq_count, block_values.shape[1], kv_local, head_size)
    scores = jnp.einsum(
        "sqhgd,skhd->shgqk", grouped, keyed_rows, preferred_element_type=jnp.float32
    ) * head_size ** (-0.5)
    capped = soft_cap * jnp.tanh(scores / soft_cap)
    spread = query_pos[:, None] - key_pos[None, :]
    live_mask = (spread >= 0) & (spread < WINDOW) & (key_pos[None, :] >= 0)
    weights = jnp.where(live_mask, jnp.exp(capped), jnp.zeros_like(capped))
    denominator = denominator + jnp.sum(weights, axis=-1)
    numerator = numerator + jnp.einsum(
        "shgqk,skhd->sqhgd",
        weights.astype(jnp.bfloat16),
        valued_rows,
        preferred_element_type=jnp.float32,
    )
    return (numerator, denominator)


def reorder_blocks(blocked, ordering):
    return blocked[ordering]


def local(queries, key_rows, value_rows, residual, out_weight, post_scale, lengths, owners):
    seq_count, shard_len, query_width = queries.shape
    seq_size = lax.axis_size("seq")
    if (
        seq_count == 1 and lax.axis_size("tp") == 4 and seq_size % 2 == 0 and seq_size >= 8
        and seq_size * shard_len <= WINDOW and key_rows.shape[2] == 2 * HD
        and shard_len % LANES == 0
    ):
        return fused(
            seq_size, queries, key_rows, value_rows, residual, out_weight, post_scale, lengths,
            owners,
        )
    kv_width = key_rows.shape[2]
    kv_local = kv_width // HD
    group_size = query_width // kv_width
    grouped = queries.reshape(seq_count, shard_len, kv_local, group_size, HD)
    position = lax.axis_index("seq")
    seq_devices = lax.axis_size("seq")
    offsets = jnp.arange(shard_len, dtype=jnp.int32)
    query_pos = position * shard_len + offsets
    numerator = jnp.zeros((seq_count, shard_len, kv_local, group_size, HD), jnp.float32)
    denominator = jnp.zeros((seq_count, kv_local, group_size, shard_len), jnp.float32)
    state_pair = attend_block(
        grouped, key_rows, value_rows, query_pos, query_pos, (numerator, denominator)
    )
    hop_count = min(WINDOW // shard_len, seq_devices - 1)
    arrived = []
    current = (key_rows, value_rows)
    for hop_index in range(1, hop_count + 1):
        current = shifted((current[0], current[1]), "seq", 1)
        arrived.append((hop_index, current))
        if len(arrived) == 2 or hop_index == hop_count:
            ordered = arrived[::-1]
            block_keys = jnp.concatenate([member[1][0] for member in ordered], axis=1)
            block_values = jnp.concatenate([member[1][1] for member in ordered], axis=1)
            block_pos = jnp.concatenate(
                [(position - member[0]) * shard_len + offsets for member in ordered]
            )
            state_pair = attend_block(
                grouped, block_keys, block_values, query_pos, block_pos, state_pair
            )
            arrived = []
    numerator, denominator = state_pair
    attended = (numerator / jnp.transpose(denominator, (0, 3, 1, 2))[..., None]).astype(
        jnp.bfloat16
    )
    partial_value = jnp.dot(
        attended.reshape(seq_count * shard_len, query_width),
        out_weight,
        preferred_element_type=jnp.float32,
    )
    partial_value = partial_value.reshape(seq_count, shard_len, out_weight.shape[1])
    branch = lax.psum_scatter(partial_value, "tp", scatter_dimension=2, tiled=True)
    squares = lax.psum(jnp.sum(branch * branch, axis=-1), "tp")
    normed = branch * lax.rsqrt(squares / D + norm_eps)[..., None] * post_scale
    hidden_out = (residual.astype(jnp.float32) + normed).astype(jnp.bfloat16)
    block_rows = shard_len // seq_devices
    slot_span = WINDOW // shard_len
    live_rows = (query_pos[None, :] >= lengths[:, None] - WINDOW) & (
        query_pos[None, :] < lengths[:, None]
    )
    kept_keys = jnp.where(live_rows[..., None], key_rows, jnp.zeros_like(key_rows))
    kept_values = jnp.where(live_rows[..., None], value_rows, jnp.zeros_like(value_rows))
    devices = jnp.arange(seq_devices, dtype=jnp.int32)
    matches = owners[:, :, None] == devices[None, None, :]
    inverse = jnp.sum(
        jnp.where(matches, devices[None, :, None], jnp.zeros_like(devices)[None, :, None]), axis=1
    )
    outgoing_keys = jax.vmap(reorder_blocks)(
        kept_keys.reshape(seq_count, seq_devices, block_rows, kv_width), inverse
    )
    outgoing_values = jax.vmap(reorder_blocks)(
        kept_values.reshape(seq_count, seq_devices, block_rows, kv_width), inverse
    )
    incoming = (
        lax.all_to_all(outgoing_keys, "seq", split_axis=1, concat_axis=1, tiled=True),
        lax.all_to_all(outgoing_values, "seq", split_axis=1, concat_axis=1, tiled=True),
    )
    selector = (
        devices[None, :] % slot_span == jnp.arange(slot_span, dtype=jnp.int32)[:, None]
    ).astype(jnp.bfloat16)
    cache_keys = (
        jnp.einsum("md,sdbf->smbf", selector, incoming[0], preferred_element_type=jnp.float32)
        .astype(jnp.bfloat16)
        .reshape(seq_count, slot_span * block_rows, kv_width)
    )
    cache_values = (
        jnp.einsum("md,sdbf->smbf", selector, incoming[1], preferred_element_type=jnp.float32)
        .astype(jnp.bfloat16)
        .reshape(seq_count, slot_span * block_rows, kv_width)
    )
    return (hidden_out, cache_keys, cache_values)


def layer_kernel(
    n, q_hbm, k_hbm, v_hbm, res_hbm, scale_hbm, len_ref, own_hbm, w_ref,
    hid_ref, ck_ref, cv_ref,
    qall, qpart, res_ref, scale_ref, own_ref, kv, other,
    down_out, down_in, pair_out, pair_in, line_out, line_in, skew_out,
    wbuf, acc, den, rounded, att, att_out, lent_out,
    to_sib, to_x, to_sib2, from_sib, from_x, from_sib2, early, total, folds, sq_out, sq_in,
    in_sem, w_sem, y_send, yq_send, y_recv, z_send, z_recv, lend_recv, q_send, q_recv, lent_send,
    down_send, down_recv, pair_send, pair_recv, line_send, line_recv, skew_send, att_send, att_recv,
    rs_send, rs_recv, sib2_recv, sq_send, sq_recv, turn, lower, upper,
):
    nz = n // 2
    top = nz - 1
    me = lax.axis_index("seq")
    t = lax.axis_index("tp")
    z, y = me // 2, me % 2
    x, c = t // 2, t % 2
    sib = x * 2 + (1 - c)
    across = (1 - x) * 2 + c
    diagonal = (1 - x) * 2 + (1 - c)
    partner = z * 2 + (1 - y)
    shard = kv.shape[2]
    width = res_ref.shape[1]
    group_cols = qpart.shape[1]
    group = group_cols // HD
    block_rows = shard // n
    chunks = shard // ROWS
    merge = LANES // ROWS
    lends = (c == 1) & (z == top)
    hosts = (c == 1) & (z == top - 1)
    takes_kv = (z < top) | (c == 0)
    sends_kv = (z < top - 1) | ((z < top) & (c == 0))

    frees = (c == 0) & (z == top - 2)
    defers = (c == 1) & (z == top - 2)

    def half(ref, which, cols):
        return ref.at[:, pl.ds(pl.multiple_of(which * cols, cols), cols)]

    loads = [
        pltpu.make_async_copy(src, dst, in_sem.at[i])
        for i, (src, dst) in enumerate(
            (
                (half(k_hbm, 1 - y, HD), other.at[0]), (half(v_hbm, 1 - y, HD), other.at[1]),
                (half(k_hbm, y, HD), kv.at[me, 0]), (half(v_hbm, y, HD), kv.at[me, 1]),
                (half(q_hbm, 1 - y, group_cols), qpart), (half(q_hbm, y, group_cols), qall.at[y]),
                (own_hbm, own_ref), (res_hbm, res_ref), (scale_hbm, scale_ref),
            )
        )
    ]
    for load in loads[:7]:
        load.start()

    barrier = pltpu.get_barrier_semaphore()
    for peer in (sib, across, diagonal):
        pl.semaphore_signal(barrier, inc=1, device_id={"tp": peer}, device_id_type=MESH)
    pl.semaphore_signal(barrier, inc=1, device_id={"seq": partner}, device_id_type=MESH)
    for there, peer in ((z < top, me + 2), (z > 0, me - 2)):

        @pl.when(there)
        def _():
            pl.semaphore_signal(barrier, inc=1, device_id={"seq": peer}, device_id_type=MESH)

    def clear(s, carry):
        acc[s] = jnp.zeros(acc.shape[1:], jnp.float32)
        den[s] = jnp.zeros(den.shape[1:], jnp.float32)
        return carry

    lax.fori_loop(0, acc.shape[0], clear, 0)
    pl.semaphore_wait(barrier, 4 + jnp.where(z < top, 1, 0) + jnp.where(z > 0, 1, 0))

    def remote(src, dst, send, recv, to):
        return pltpu.make_async_remote_copy(
            src_ref=src, dst_ref=dst, send_sem=send, recv_sem=recv, device_id=to,
            device_id_type=MESH,
        )

    def settle(ref, sem):
        pltpu.make_async_copy(ref, ref, sem.at[0]).wait()

    def y_copy(h, origin):
        return remote(
            other.at[h], kv.at[origin, h], y_send.at[0], y_recv.at[h], {"seq": partner}
        )

    def yq_copy(slot):
        return remote(qpart, qall.at[slot], yq_send.at[0], y_recv.at[2], {"seq": partner})

    def z_copy(origin, h):
        return remote(
            kv.at[origin, h], kv.at[origin, h], z_send.at[0], z_recv.at[origin, h],
            {"seq": me + 2},
        )

    def lend_copy(yq):
        return remote(
            qall.at[yq], qall.at[2 + yq], q_send.at[0], q_recv.at[0], {"seq": me - 2}
        )

    def lend_kv(origin, h):
        return remote(
            kv.at[origin, h], kv.at[origin, h], z_send.at[0], lend_recv.at[0],
            {"seq": me - 2},
        )

    def w_copy(f, g):
        return pltpu.make_async_copy(
            w_ref.at[pl.ds(g * group_cols, group_cols), pl.ds(f * width, width)],
            wbuf.at[f, g], w_sem.at[0],
        )

    for h in (0, 1):
        loads[2 + h].wait()
        pl.when(sends_kv)(z_copy(me, h).start)
    for load in (loads[0], loads[1], loads[4], loads[5]):
        load.wait()

    @pl.when(z == top)
    def _():
        yq_copy(y).start()
        for h in (0, 1):
            y_copy(h, me).start()

    @pl.when(z < top)
    def _():
        for h in (0, 1):
            y_copy(h, me).start()
        yq_copy(y).start()

    @pl.when(lends)
    def _():
        lend_copy(y).start()
        for h in (0, 1):
            lend_kv(me, h).start()

    loads[6].wait()
    for f in range(4):
        for g in (0, 1):
            w_copy(f, g).start()
    for load in loads[7:]:
        load.start()

    @pl.when(z > 0)
    def _():
        pl.semaphore_wait(lower, 1)

    @pl.when(z < top)
    def _():
        pl.semaphore_signal(lower, inc=1, device_id={"seq": me + 2}, device_id_type=MESH)

    @pl.when(lends)
    def _():
        pl.semaphore_signal(upper, inc=1, device_id={"seq": me - 2}, device_id_type=MESH)

    def owned(device):
        block = own_ref[0, 0] * 0
        for b in range(n):
            block = block + jnp.where(own_ref[0, b] == device, b, 0)
        return jnp.full((block_rows, HD), block, jnp.int32)

    def select(ref, lead, chosen):
        got = jnp.zeros(chosen.shape, jnp.float32)
        for b in range(n):
            rows = ref[(*lead, slice(b * block_rows, (b + 1) * block_rows))]
            got = jnp.where(chosen == b, rows.astype(jnp.float32), got)
        return got.astype(jnp.bfloat16)

    def down_copy(to, slot):
        return remote(
            down_out.at[to], down_in.at[slot], down_send.at[0], down_recv.at[0], {"seq": to}
        )

    def stage(to, carry):
        chosen = owned(to)
        for h in (0, 1):
            down_out[to, h, y] = select(kv, (me, h), chosen)
            down_out[to, h, 1 - y] = select(other, (h,), chosen)
        return carry

    def post(to, carry):
        down_copy(to, me).start()
        return carry

    lax.fori_loop(0, 2 * z, stage, 0)

    def pair_copy(zo):
        return remote(
            pair_out.at[zo], pair_in.at[zo], pair_send.at[0], pair_recv.at[0], {"seq": partner}
        )

    def line_copy(zo):
        return remote(
            line_out.at[zo], line_in.at[zo], line_send.at[0], line_recv.at[0], {"seq": me + 2}
        )

    def skew_copy(zo):
        return remote(
            skew_out.at[zo], pair_in.at[zo], skew_send.at[0], pair_recv.at[0],
            {"seq": partner + 2},
        )

    def gather(zo, device, out):
        chosen = owned(device)
        for yo in (0, 1):
            for h in (0, 1):
                out[zo, yo, h] = select(kv, (2 * zo + yo, h), chosen)

    def pass_cache(zo):
        @pl.when((zo == z) | takes_kv)
        def _():
            gather(zo, partner, pair_out)
            pair_copy(zo).start()

    def lift_cache(zo):
        gather(zo, me + 2, line_out)
        line_copy(zo).start()
        gather(zo, partner + 2, skew_out)
        skew_copy(zo).start()

    @pl.when(lends)
    def _():
        yq_copy(1 - y).wait_recv()
        lend_copy(1 - y).start()

    for h in (0, 1):
        y_copy(h, partner).wait_recv()
        pl.when(sends_kv)(z_copy(partner, h).start)
        pl.when(lends)(lend_kv(partner, h).start)
    lax.fori_loop(0, 2 * z, post, 0)

    @pl.when(hosts)
    def _():
        pl.semaphore_wait(upper, 1)
        lift_cache(z)

    def take(origin, h):
        z_copy(origin, h).wait_recv()
        held_back = defers & (origin == 1 - y)
        pl.when(sends_kv & jnp.logical_not(held_back))(z_copy(origin, h).start)

    @pl.when((z > 0) & takes_kv)
    def _():
        for origin in (me - 2, partner - 2):
            for h in (0, 1):
                take(origin, h)

    @pl.when(hosts & (z > 1))
    def _():
        lift_cache(z - 1)

    @pl.when(jnp.logical_not(lends))
    def _():
        yq_copy(1 - y).wait_recv()

    def attend(base, origin, above):
        pair = pl.ds(base, 2)
        for hh in range(group):
            stacked = qall[pair, :, hh * HD : (hh + 1) * HD].reshape(2 * shard, HD)
            scores = lax.dot_general(
                stacked, kv[origin, 0], (((1,), (1,)), ((), ())),
                preferred_element_type=jnp.float32,
            )
            w = jnp.exp2(jnp.tanh(scores * (HD ** (-0.5) / soft_cap)) * (soft_cap * LOG2E))
            if above is not None:
                keep = lax.broadcasted_iota(jnp.int32, w.shape, 0) >= above + (
                    lax.broadcasted_iota(jnp.int32, w.shape, 1)
                )
                w = jnp.where(keep, w, 0.0)
            folded = w[:, :LANES]
            for i in range(1, w.shape[1] // LANES):
                folded = folded + w[:, i * LANES : (i + 1) * LANES]
            den[hh, pair] += folded.reshape(2, shard, LANES)
            acc[hh, pair] += jnp.dot(
                w.astype(jnp.bfloat16), kv[origin, 1], preferred_element_type=jnp.float32
            ).reshape(2, shard, HD)

    def weigh(i, origin):
        pair = pl.ds(2 * i, 2)
        for hh in range(group):
            stacked = qall[pair, :, hh * HD : (hh + 1) * HD].reshape(2 * shard, HD)
            scores = lax.dot_general(
                stacked, kv[origin, 0], (((1,), (1,)), ((), ())),
                preferred_element_type=jnp.float32,
            )
            w = jnp.exp2(jnp.tanh(scores * (HD ** (-0.5) / soft_cap)) * (soft_cap * LOG2E))
            folded = w[:, :LANES]
            for j in range(1, w.shape[1] // LANES):
                folded = folded + w[:, j * LANES : (j + 1) * LANES]
            den[hh, pair] += folded.reshape(2, shard, LANES)
            rounded[i, hh] = w.astype(jnp.bfloat16)

    def mix(i, origin):
        pair = pl.ds(2 * i, 2)
        for hh in range(group):
            acc[hh, pair] += jnp.dot(
                rounded[i, hh], kv[origin, 1], preferred_element_type=jnp.float32
            ).reshape(2, shard, HD)

    def invert():
        def one(i, carry):
            pair = pl.ds(2 * i, 2)
            for hh in range(group):
                whole = den[hh, pair].reshape(2 * shard, LANES)
                inverse = 1.0 / jnp.sum(whole, axis=-1, keepdims=True)
                den[hh, pair] = jnp.broadcast_to(inverse, whole.shape).reshape(2, shard, LANES)
            return carry

        lax.fori_loop(0, jnp.where(hosts, 2, 1), one, 0)

    def own_slab(base, slab):
        def diagonal_block(i, carry):
            attend(base, 2 * slab + i, i * shard)
            return carry

        lax.fori_loop(0, 2, diagonal_block, 0)

    pl.when(jnp.logical_not(lends))(functools.partial(own_slab, 0, z))
    @pl.when(hosts)
    def _():
        settle(qall.at[2:], q_recv)

        def one(i, carry):
            attend(2, 2 * z + i, None)
            return carry

        lax.fori_loop(0, 2, one, 0)

    def rows_of(r):
        return pl.ds(pl.multiple_of(r * ROWS, ROWS), ROWS)

    def att_copy(r, g):
        return remote(
            att_out.at[r], att.at[g, r], att_send.at[0], att_recv.at[r], {"seq": partner}
        )

    def lent_copy(yq, r, g):
        return remote(
            lent_out.at[yq, r], att.at[g, r], lent_send.at[0], att_recv.at[r],
            {"seq": 2 * top + yq},
        )

    def finish(s, r, out, lead):
        for hh in range(group):
            for i in range(HD // LANES):
                cols = slice(i * LANES, (i + 1) * LANES)
                out[(*lead, slice(None), slice(hh * HD + i * LANES, hh * HD + (i + 1) * LANES))] = (
                    acc[hh, s, rows_of(r), cols] * den[hh, s, rows_of(r), :]
                ).astype(jnp.bfloat16)

    def give(r, carry):
        for yq in (1 - y, y):
            finish(2 + yq, r, lent_out, (yq, r))
            lent_copy(yq, r, y).start()
        return carry

    pairs = jnp.where(hosts, 2, 1)

    def phase(d, carry):
        @pl.when(z - d + 1 >= 1)
        def _():
            pass_cache(z - d + 1)

        @pl.when(hosts & (d > 2) & (z - d + 1 >= 1))
        def _():
            lift_cache(z - d + 1)

        @pl.when(hosts & (d == jnp.minimum(2, z)))
        def _():
            settle(kv.at[2 * top :], lend_recv)
            own_slab(2, top)

        def side(j, carry):
            @pl.when((z - d >= 0) & takes_kv)
            def _():
                origin = 2 * (z - d) + jnp.where(j == 0, y, 1 - y)
                for h, work in enumerate((weigh, mix)):
                    pl.when(d > 1)(functools.partial(take, origin, h))

                    def one(i, carry):
                        which = pairs - 1 - i
                        work(which, origin)
                        if h == 1:

                            @pl.when((which == 1) & (d == z) & (j == 1))
                            def _():
                                lax.fori_loop(0, chunks, give, 0)

                        return carry

                    lax.fori_loop(0, pairs, one, 0)
                    if h == 0:
                        pl.when((d == z) & (j == 1))(invert)

            return carry

        lax.fori_loop(0, 2, side, 0)
        return carry

    lax.fori_loop(1, nz, phase, 0)

    pl.when(z == 0)(invert)

    @pl.when(frees)
    def _():
        settle(kv.at[: 2 * top - 2], z_send)
        pl.semaphore_signal(turn, inc=1, device_id={"tp": sib}, device_id_type=MESH)

    @pl.when(defers)
    def _():
        pl.semaphore_wait(turn, 1)
        for h in (0, 1):
            z_copy(1 - y, h).start()

    def away(r, carry):
        finish(1 - y, r, att_out, (r,))
        att_copy(r, y).start()
        return carry

    def home(r, carry):
        finish(y, r, att, (y, r))
        return carry

    @pl.when(jnp.logical_not(lends))
    def _():
        lax.fori_loop(0, chunks, away, 0)
        lax.fori_loop(0, chunks, home, 0)

    def rs_copy(kind, r, src, dst, recv, to):
        return remote(src.at[r], dst.at[r], rs_send.at[kind], recv, {"tp": to})

    def sib_copy(r):
        return rs_copy(0, r, to_sib, from_sib, rs_recv.at[0, r], sib)

    def x_copy(r):
        return rs_copy(1, r, to_x, from_x, rs_recv.at[1, r], across)

    def sib2_copy(r):
        return rs_copy(2, r, to_sib2, from_sib2, sib2_recv.at[0], sib)

    def product(rows, f, g):
        return jnp.dot(rows, wbuf[f, g], preferred_element_type=jnp.float32)

    def part(f, r):
        some = pl.ds(merge * r, merge)
        rows = [att[g, some].reshape(LANES, group_cols) for g in (0, 1)]
        return product(rows[0], f, 0) + product(rows[1], f, 1)

    settle(wbuf, w_sem)

    sent = (diagonal, across)

    @pl.when(jnp.logical_not(lends))
    def _():
        for i, f in enumerate(sent):
            early[i] = product(att[y].reshape(shard, group_cols), f, y)

    def send_sib(r):
        pl.when(jnp.logical_not(lends))(att_copy(r, 1 - y).wait_recv)

        @pl.when(lends)
        def _():
            both_heads = att.at[:, r]
            pltpu.make_async_copy(both_heads, both_heads, att_recv.at[r]).wait()
            early[0, rows_of(r), :] = product(att[y, r], diagonal, y)

        to_sib[r] = (early[0, rows_of(r), :] + product(att[1 - y, r], diagonal, 1 - y)).astype(
            jnp.bfloat16
        )
        sib_copy(r).start()

    def send_x(r):
        @pl.when(lends)
        def _():
            early[1, rows_of(r), :] = product(att[y, r], across, y)

        mine = early[1, rows_of(r), :] + product(att[1 - y, r], across, 1 - y)
        sib_copy(r).wait_recv()
        to_x[r] = (mine + from_sib[r].astype(jnp.float32)).astype(jnp.bfloat16)
        x_copy(r).start()

    def both(r, carry):
        pl.when(r < chunks)(functools.partial(send_sib, r))
        pl.when(r > 0)(functools.partial(send_x, r - 1))
        return carry

    def third(r, carry):
        some = pl.ds(merge * r, merge)
        to_sib2[some] = part(sib, r).astype(jnp.bfloat16).reshape(merge, ROWS, width)
        for i in range(merge):
            sib2_copy(merge * r + i).start()
        return carry

    def fourth(r, carry):
        rows = pl.ds(pl.multiple_of(r * LANES, LANES), LANES)
        total[rows, :] = part(t, r)
        return carry

    lax.fori_loop(0, chunks + 1, both, 0)

    pass_cache(0)
    pl.when(hosts)(functools.partial(lift_cache, 0))

    for step in (third, fourth):
        lax.fori_loop(0, chunks // merge, step, 0)

    mine_blocks = owned(me)
    local_row = lax.broadcasted_iota(jnp.int32, mine_blocks.shape, 0)
    bound = jnp.full(mine_blocks.shape, len_ref[0], jnp.int32)

    for slab in range(nz):

        @pl.when(z == slab)
        def _():
            settle(pair_in.at[: slab + 1], pair_recv)
            if slab < top:
                settle(down_in.at[2 * slab + 2 :], down_recv)

    @pl.when(lends)
    def _():
        settle(line_in.at[:top], line_recv)

    def cache(zo, carry):
        far = lends & (zo < top)

        for yo in (0, 1):
            origin = 2 * zo + yo
            pos = local_row + mine_blocks * block_rows + origin * shard
            live = (pos < bound) & (pos >= bound - WINDOW)
            rows = pl.ds(pl.multiple_of(origin * block_rows, block_rows), block_rows)

            for h, out in enumerate((ck_ref, cv_ref)):

                def put(g, value):
                    cols = pl.ds(pl.multiple_of(g * HD, HD), HD)
                    out[rows, cols] = jnp.where(live, value.astype(jnp.float32), 0.0).astype(
                        jnp.bfloat16
                    )

                @pl.when(zo > z)
                def _():
                    for g in (0, 1):
                        put(g, down_in[origin, h, g])

                @pl.when(zo <= z)
                def _():
                    put(1 - y, pair_in[zo, yo, h])

                @pl.when((zo <= z) & jnp.logical_not(far))
                def _():
                    put(y, select(kv, (origin, h), mine_blocks))

                @pl.when(far)
                def _():
                    put(y, line_in[zo, yo, h])

        return carry

    lax.fori_loop(0, nz, cache, 0)
    rest = ck_ref.shape[0] - n * block_rows
    if rest:
        for out in (ck_ref, cv_ref):
            out[n * block_rows :, :] = jnp.zeros((rest, 2 * HD), jnp.bfloat16)
    settle(from_sib2, sib2_recv)
    for r in range(chunks):
        x_copy(r).wait_recv()
        rows = slice(r * ROWS, (r + 1) * ROWS)
        branch = total[rows, :] + from_sib2[r].astype(jnp.float32) + from_x[r].astype(jnp.float32)
        total[rows, :] = branch
        squared = branch * branch
        folded = squared[:, :LANES]
        for i in range(1, width // LANES):
            folded = folded + squared[:, i * LANES : (i + 1) * LANES]
        folds[rows, :] = folded
        if (r + 1) * ROWS % LANES == 0:
            rows = slice((r + 1) * ROWS - LANES, (r + 1) * ROWS)
            line = jnp.sum(folds[rows, :].T, axis=0, keepdims=True)
            sq_out[:, rows] = jnp.broadcast_to(line, (8, LANES))

    def sq_copy(i, to, slot):
        return pltpu.make_async_remote_copy(
            src_ref=sq_out, dst_ref=sq_in.at[slot], send_sem=sq_send.at[0],
            recv_sem=sq_recv.at[0], device_id={"tp": to}, device_id_type=MESH,
        )

    peers = (sib, across, diagonal)
    for i, peer in enumerate(peers):
        sq_copy(i, peer, t).start()
    squares = sq_out[...]
    settle(sq_in.at[:3], sq_recv)
    for i, peer in enumerate(peers):
        squares = squares + sq_in[peer]
    loads[7].wait()
    loads[8].wait()
    factor = lax.rsqrt(squares / D + norm_eps)
    for r in range(shard // LANES):
        rows = slice(r * LANES, (r + 1) * LANES)
        spread = jnp.broadcast_to(factor[:1, rows], (LANES, LANES)).T
        for i in range(width // LANES):
            cols = slice(i * LANES, (i + 1) * LANES)
            normed = total[rows, cols] * spread * scale_ref[cols].reshape(1, LANES)
            hid_ref[rows, cols] = (res_ref[rows, cols].astype(jnp.float32) + normed).astype(
                jnp.bfloat16
            )

    settle(sq_in.at[:3], sq_send)
    for kind, sent_rows in enumerate((to_sib, to_x, to_sib2)):
        pltpu.make_async_copy(sent_rows, sent_rows, rs_send.at[kind]).wait()
    settle(other, y_send)
    settle(qpart, yq_send)
    for slab in range(nz):

        @pl.when((z == slab) & sends_kv & jnp.logical_not(frees))
        def _():
            settle(kv.at[: 2 * slab + 2], z_send)

        @pl.when((z == slab) & takes_kv)
        def _():
            settle(pair_out.at[: slab + 1], pair_send)

        if slab:

            @pl.when(z == slab)
            def _():
                settle(down_out.at[: 2 * slab], down_send)

    @pl.when(lends)
    def _():
        settle(qall.at[:2], q_send)
        settle(kv.at[2 * top :], z_send)
        settle(pair_out.at[top:], pair_send)

    @pl.when(jnp.logical_not(lends))
    def _():
        settle(att_out, att_send)

    @pl.when(hosts)
    def _():
        settle(lent_out, lent_send)
        settle(line_out.at[:top], line_send)
        settle(skew_out.at[:top], skew_send)


def put_out(*refs):
    count = (len(refs) - 1) // 2
    sems = refs[-1]
    for i in range(count):
        src, dst = refs[i], refs[count + i]
        step = src.shape[0] // PIECES
        for k in range(PIECES):
            rows = pl.ds(k * step, step)
            pltpu.make_async_copy(src.at[rows], dst.at[rows], sems.at[i]).start()
    for i in range(count):
        pltpu.make_async_copy(refs[i], refs[count + i], sems.at[i]).wait()


def fused(n, queries, key_rows, value_rows, residual, out_weight, post_scale, lengths, owners):
    shard, q_width = queries.shape[1:]
    kv_width = key_rows.shape[2]
    width = residual.shape[2]
    chunks = shard // ROWS
    cache_rows = WINDOW // n
    smem = pl.BlockSpec(memory_space=pltpu.SMEM)
    apart = pl.BlockSpec(memory_space=pl.ANY)
    held = pl.BlockSpec(memory_space=pltpu.VMEM)
    one = pltpu.SemaphoreType.DMA((1,))
    group_cols = q_width * HD // kv_width
    slab = pltpu.VMEM((n // 2, 2, 2, shard // n, HD), jnp.bfloat16)
    half = pltpu.VMEM((chunks, ROWS, width), jnp.bfloat16)
    hidden, ck, cv = pl.pallas_call(
        functools.partial(layer_kernel, n),
        out_shape=(
            pltpu.VMEM((shard, width), jnp.bfloat16),
            pltpu.VMEM((cache_rows, kv_width), jnp.bfloat16),
            pltpu.VMEM((cache_rows, kv_width), jnp.bfloat16),
        ),
        in_specs=[apart] * 5 + [smem] + [apart] * 2,
        out_specs=(held,) * 3,
        scratch_shapes=[
            pltpu.VMEM((4, shard, group_cols), jnp.bfloat16),
            pltpu.VMEM((shard, group_cols), jnp.bfloat16),
            pltpu.VMEM((shard, width), jnp.bfloat16),
            pltpu.VMEM((width,), jnp.float32),
            pltpu.SMEM((1, n), jnp.int32),
            pltpu.VMEM((n, 2, shard, HD), jnp.bfloat16),
            pltpu.VMEM((2, shard, HD), jnp.bfloat16),
            pltpu.VMEM((n, 2, 2, shard // n, HD), jnp.bfloat16),
            pltpu.VMEM((n, 2, 2, shard // n, HD), jnp.bfloat16),
            slab, slab, slab, slab, slab,
            pltpu.VMEM((4, 2, group_cols, width), jnp.bfloat16),
            pltpu.VMEM((group_cols // HD, 4, shard, HD), jnp.float32),
            pltpu.VMEM((group_cols // HD, 4, shard, LANES), jnp.float32),
            pltpu.VMEM((2, group_cols // HD, 2 * shard, HD), jnp.bfloat16),
            pltpu.VMEM((2, chunks, ROWS, group_cols), jnp.bfloat16),
            pltpu.VMEM((chunks, ROWS, group_cols), jnp.bfloat16),
            pltpu.VMEM((2, chunks, ROWS, group_cols), jnp.bfloat16),
            half, half, half, half, half, half,
            pltpu.VMEM((2, shard, width), jnp.float32),
            pltpu.VMEM((shard, width), jnp.float32),
            pltpu.VMEM((shard, LANES), jnp.float32),
            pltpu.VMEM((8, shard), jnp.float32),
            pltpu.VMEM((4, 8, shard), jnp.float32),
            pltpu.SemaphoreType.DMA((9,)),
            one,
            one,
            one,
            pltpu.SemaphoreType.DMA((3,)),
            one,
            pltpu.SemaphoreType.DMA((n - 2, 2)),
            one,
            one,
            one,
            one,
            one,
            one,
            one,
            one,
            one,
            one,
            one,
            one,
            pltpu.SemaphoreType.DMA((chunks,)),
            pltpu.SemaphoreType.DMA((3,)),
            pltpu.SemaphoreType.DMA((2, chunks)),
            one,
            one,
            one,
            pltpu.SemaphoreType.REGULAR,
            pltpu.SemaphoreType.REGULAR,
            pltpu.SemaphoreType.REGULAR,
        ],
        compiler_params=pltpu.CompilerParams(
            collective_id=0, has_side_effects=True, vmem_limit_bytes=62 * 1024 * 1024
        ),
    )(
        queries[0], key_rows[0], value_rows[0], residual[0], post_scale, lengths, owners,
        out_weight,
    )
    made = (hidden, ck, cv)
    hidden, ck, cv = pl.pallas_call(
        put_out,
        out_shape=tuple(jax.ShapeDtypeStruct(a.shape, a.dtype) for a in made),
        in_specs=[apart] * len(made),
        out_specs=(apart,) * len(made),
        scratch_shapes=[pltpu.SemaphoreType.DMA((len(made),))],
    )(*(pltpu.with_memory_space_constraint(a, pltpu.VMEM) for a in made))
    return hidden[None], ck[None], cv[None]


def solution(mesh):
    placed = (
        P(None, "seq", "tp"),
        P(None, "seq", "tp"),
        P(None, "seq", "tp"),
        P(None, "seq", "tp"),
        P("tp", None),
        P("tp"),
        P(),
        P(),
    )
    return jax.shard_map(
        local,
        mesh=mesh,
        in_specs=placed,
        out_specs=(P(None, "seq", "tp"), P(None, "seq", "tp"), P(None, "seq", "tp")),
        check_vma=False,
    )
```
